256 devices in a mesh: groups: 4 (over x, y), space: 64 (over z, core).
Axes of the slice: x: 2, y: 2, z: 32, core: 2. Of those that a mesh axis runs over, the one named last changes fastest.
The devices are a block of a 4x8x32 slice.
Arguments:
- inputs: bfloat16 [1536, 1152, 256], P(('groups', 'space')), parts along dimension 0, may hold values from -6 to 6
- spectral_weight: bfloat16 [2, 256, 2, 256, 256], P(None, 'space'), may hold values from -0.25 to 0.25
- local_weight: bfloat16 [2, 256, 256], replicated, may hold values from -0.375 to 0.375
- layer_bias: bfloat16 [2, 256], replicated, may hold values from -3 to 3
- readout_hidden: bfloat16 [256, 256], replicated, may hold values from -0.375 to 0.375
- readout_final: bfloat16 [20, 256], replicated, may hold values from -0.375 to 0.375
Outputs:
- forecast: bfloat16 [20, 1536, 1152], P(None, ('groups', 'space')), parts along dimension 1
The draws below stay inside these ranges and needn't reach their ends.
There are 4 independent parts, one for each index of `groups`. The reference program is written for one: setup_inputs(seed, part) draws one part's arguments, and reference() takes and returns one part's arrays. A program takes and returns all parts, laid end to end along the dimension named above; an argument that names none is the same for every part. Nothing has to cross between parts.
All inputs are finite; a program needn't handle non-finite values.
Results may differ from the reference program's by a relative error of at most 0.018.
Values may be sent and summed in bfloat16 or wider, within the bound.
A program may use at most 64 MiB of HBM per device.

```python
import jax
import jax.numpy as jnp
from jax import lax

H = 384
W = 1152
C = 256
KY = 16
KX = 16
LAYERS = 2
QH = 256
VARS = 20
MODES = 256
N_SPACE = 64


def block_scale(rng, extent, cuts, smallest, top_value):
    gain, own = 1.0, jax.random.fold_in(rng, 6)
    for axis_at, blocks in cuts:
        heights = jnp.exp(jax.random.uniform(jax.random.fold_in(own, axis_at), (blocks,), jnp.float32, smallest / len(cuts), top_value / len(cuts)))
        gain = gain * jnp.repeat(heights, extent[axis_at] // blocks).reshape([-1 if axis == axis_at else 1 for axis in range(len(extent))])
    return gain


def gaussian(rng, extent, scale, reach, cuts=(), kind=jnp.bfloat16):
    drawn = jax.random.normal(rng, extent, jnp.float32) * scale
    if len(cuts) > 0:
        drawn = block_scale(rng, extent, cuts, -0.22, 0.18) * drawn
    return jnp.clip(drawn, min=-reach, max=reach).astype(kind)


def setup_inputs(seed: int = 0, part: int = 0) -> dict:
    key_list = jax.random.split(jax.random.key(seed), 7)
    own_keys = jax.random.split(jax.random.fold_in(key_list[6], part), 7)
    return {
        "inputs": gaussian(own_keys[0], (H, W, C), 1.0, 6.0, ((0, 64),)),
        "spectral_weight": gaussian(key_list[1], (LAYERS, MODES, 2, C, C), (2 * C) ** -0.5, 0.25, ((1, 64),)),
        "local_weight": gaussian(key_list[2], (LAYERS, C, C), C ** -0.5, 0.375),
        "layer_bias": gaussian(key_list[3], (LAYERS, C), 0.5, 3.0),
        "readout_hidden": gaussian(key_list[4], (C, QH), C ** -0.5, 0.375),
        "readout_final": gaussian(key_list[5], (VARS, QH), QH ** -0.5, 0.375),
    }


def zonal_tables(columns, modes):
    column_ids = jnp.arange(columns, dtype=jnp.int32)
    wave_numbers = jnp.arange(1, modes + 1, dtype=jnp.int32)
    phase_int = column_ids[:, None] * wave_numbers[None, :] % columns
    angles = 2.0 * jnp.pi / columns * phase_int.astype(jnp.float32)
    cosines = jnp.cos(angles)
    sines = jnp.sin(angles)
    forward = jnp.concatenate([cosines, -sines], axis=1) / jnp.sqrt(jnp.float32(columns))
    inverse = jnp.stack([cosines, -sines], axis=2).reshape(columns, 2 * modes) * jnp.sqrt(jnp.float32(2.0 / modes))
    return (forward.astype(jnp.bfloat16), inverse.astype(jnp.bfloat16))

def meridional_tables(row_ids, height, modes):
    mode_index = jnp.arange(modes, dtype=jnp.int32)
    wave_numbers = jnp.where(mode_index < modes // 2, mode_index, mode_index - modes)
    phase_int = wave_numbers[:, None] * row_ids[None, :] % height
    angles = 2.0 * jnp.pi / height * phase_int.astype(jnp.float32)
    cosines = jnp.cos(angles)
    sines = jnp.sin(angles)
    forward = jnp.stack([jnp.stack([cosines, sines], axis=2), jnp.stack([-sines, cosines], axis=2)], axis=1)
    forward = forward / jnp.sqrt(jnp.float32(height))
    cos_rows = cosines.T
    sin_rows = sines.T
    inverse = jnp.stack([jnp.stack([cos_rows, -sin_rows], axis=2), jnp.stack([sin_rows, cos_rows], axis=2)], axis=1)
    inverse = inverse / jnp.sqrt(jnp.float32(modes))
    return (forward.astype(jnp.bfloat16), inverse.astype(jnp.bfloat16))

def mix_modes(spectrum, weights):
    real_in = spectrum[:, 0].astype(jnp.float32)
    imag_in = spectrum[:, 1].astype(jnp.float32)
    real_weight = weights[:, 0].astype(jnp.float32)
    imag_weight = weights[:, 1].astype(jnp.float32)

    def product(vectors, matrices):
        return jnp.einsum('mi,mio->mo', vectors, matrices)
    real_out = product(real_in, real_weight) - product(imag_in, imag_weight)
    imag_out = product(real_in, imag_weight) + product(imag_in, real_weight)
    return jnp.stack([real_out, imag_out], axis=1).astype(jnp.bfloat16)

def reference(inputs, spectral_weight, local_weight, layer_bias, readout_hidden, readout_final):
    height, columns, channels = inputs.shape
    blocks = height // 64
    zonal_forward, zonal_inverse = zonal_tables(columns, KX)
    rows_each = height // N_SPACE
    stored_rows = jnp.arange(height, dtype=jnp.int32)
    row_ids = (stored_rows % rows_each * N_SPACE + stored_rows // rows_each).astype(jnp.int32)
    meridional_forward, meridional_inverse = meridional_tables(row_ids, height, KY)
    current = inputs
    for layer_index in range(LAYERS):

        def zonal_block(block_rows):
            return jnp.einsum('hwc,wj->hjc', block_rows.astype(jnp.float32), zonal_forward.astype(jnp.float32)).astype(jnp.bfloat16)
        zonal_part = lax.map(zonal_block, current.reshape(blocks, 64, columns, channels))
        zonal_view = zonal_part.reshape(height, 2, KX, channels)
        spectrum = jnp.einsum('qphr,hrkc->qkpc', meridional_forward.astype(jnp.float32), zonal_view.astype(jnp.float32))
        spectrum = spectrum.reshape(MODES, 2, channels).astype(jnp.bfloat16)
        mixed = mix_modes(spectrum, spectral_weight[layer_index]).reshape(KY, KX, 2, channels)
        returned = jnp.einsum('hpqr,qkrc->hkpc', meridional_inverse.astype(jnp.float32), mixed.astype(jnp.float32))
        returned = returned.astype(jnp.bfloat16).reshape(blocks, 64, 2 * KX, channels)
        weight_now = local_weight[layer_index]
        bias_now = layer_bias[layer_index].astype(jnp.float32)

        def finish(block_pair):
            block_rows, block_back = block_pair
            spread = jnp.einsum('wj,hjc->hwc', zonal_inverse.astype(jnp.float32), block_back.astype(jnp.float32))
            pointwise = jnp.dot(block_rows.reshape(-1, channels), weight_now, preferred_element_type=jnp.float32)
            pointwise = pointwise.reshape(block_rows.shape)
            return jax.nn.gelu(spread + pointwise + bias_now, approximate=True).astype(jnp.bfloat16)
        current = lax.map(finish, (current.reshape(blocks, 64, columns, channels), returned))
        current = current.reshape(height, columns, channels)

    def readout(block_rows):
        flat_rows = block_rows.reshape(-1, channels)
        hidden = jax.nn.gelu(jnp.dot(flat_rows, readout_hidden, preferred_element_type=jnp.float32), approximate=True)
        hidden = hidden.astype(jnp.bfloat16)
        final = jnp.einsum('pq,nq->pn', readout_final.astype(jnp.float32), hidden.astype(jnp.float32))
        return final.astype(jnp.bfloat16).reshape(readout_final.shape[0], 64, columns)
    pieces = lax.map(readout, current.reshape(blocks, 64, columns, channels))
    return jnp.transpose(pieces, (1, 0, 2, 3)).reshape(readout_final.shape[0], height, columns)
```

```python
import functools

import jax
import jax.numpy as jnp
import numpy as np
from jax import lax
from jax.experimental import pallas as pl
from jax.experimental.pallas import tpu as pltpu
from jax.sharding import PartitionSpec as P

KY = 16
KX = 16
LAYERS = 2
MODES = KY * KX
CORES = 2
BF = jnp.bfloat16
F32 = jnp.float32
MESH = pl.DeviceIdType.MESH


def zonal_tables(columns):
    phase = np.arange(columns)[:, None] * np.arange(1, KX + 1)[None, :] % columns
    angles = np.float32(2.0 * np.pi / columns) * phase.astype(np.float32)
    cosines, sines = np.cos(angles), np.sin(angles)
    forward = np.concatenate([cosines, -sines], axis=1) / np.sqrt(np.float32(columns))
    inverse = np.stack([cosines, -sines], axis=2).reshape(columns, 2 * KX)
    inverse = inverse * np.sqrt(np.float32(2.0 / KX))
    return forward.T.astype(BF), inverse.astype(BF)


def meridional_tables(devices, rows_here):
    height = devices * rows_here
    index = np.arange(KY)
    waves = np.where(index < KY // 2, index, index - KY)
    rows = np.arange(rows_here)[None, :] * devices + np.arange(devices)[:, None]
    phase = waves[None, :, None] * rows[:, None, :] % height
    angles = np.float32(2.0 * np.pi / height) * phase.astype(np.float32)
    cosines, sines = np.cos(angles), np.sin(angles)
    forward = np.stack([np.stack([cosines, sines], -1), np.stack([-sines, cosines], -1)], 2)
    forward = forward / np.sqrt(np.float32(height))
    cos_t, sin_t = cosines.transpose(0, 2, 1), sines.transpose(0, 2, 1)
    inverse = np.stack([np.stack([cos_t, -sin_t], -1), np.stack([sin_t, cos_t], -1)], 2)
    inverse = inverse / np.sqrt(np.float32(KY))
    pairs = 2 * rows_here
    padded_f = np.zeros((devices, 2 * KY, 128), np.float32)
    padded_f[:, :, :pairs] = forward.reshape(devices, 2 * KY, pairs)
    padded_i = np.zeros((devices, -(-pairs // 16) * 16, 128), np.float32)
    padded_i[:, :pairs, : 2 * KY] = inverse.reshape(devices, pairs, 2 * KY)
    return padded_f.astype(BF), padded_i.astype(BF)


def selection_tables(devices, rows_here):
    each = MODES // devices
    chips = devices // CORES
    core, chip, one, part = np.meshgrid(
        np.arange(CORES), np.arange(chips), np.arange(each), np.arange(2), indexing="ij"
    )
    mode = ((chip * CORES + core) * each + one).reshape(-1)
    part = part.reshape(-1)
    wave_y, wave_x = mode // KX, mode % KX
    pick_mode = (wave_y * 2 + part)[:, None] == np.arange(128)[None, :]
    h, r, k = np.meshgrid(np.arange(rows_here), np.arange(2), np.arange(KX), indexing="ij")
    pick_in = np.arange(128)[:, None] == (h * 2 + r).reshape(-1)[None, :]
    mask_in = wave_x[:, None] == k.reshape(-1)[None, :]
    h, k, p = np.meshgrid(np.arange(rows_here), np.arange(KX), np.arange(2), indexing="ij")
    pairs = -(-2 * rows_here // 16) * 16
    pick_out = (h * 2 + p).reshape(-1)[:, None] == np.arange(pairs)[None, :]
    mask_out = k.reshape(-1)[:, None] == wave_x[None, :]
    tables = (pick_mode[:, : 2 * KY], pick_in, mask_in, pick_out, pick_mode.T, mask_out)
    return tuple(np.asarray(t, np.float32).astype(BF) for t in tables)


def dot(a, b):
    return jnp.dot(a, b, preferred_element_type=F32)


def gelu(v):
    half = 0.5 * v
    scale = float(np.sqrt(2.0 / np.pi))
    return half + half * jnp.tanh(v * (scale + (scale * 0.044715) * (v * v)))


def kernel(
    x_hbm, sw_hbm, lw_hbm, bias_hbm, rh_hbm, rf_hbm, zf_hbm, zi_hbm, tf_hbm, ti_hbm,
    pm_hbm, pin_hbm, min_hbm, pout_hbm, pmt_hbm, mout_hbm,
    out_ref,
    state, sw, lw, bias, rh, rf, zf, zi, tf, ti, pm, pin, minn, pout, pmt, mout,
    m2, n2, zonal, pw, returned, xsend, xrecv, pbuf, rbuf, mall,
    in_sem, sw_sem, small_sem, late_sem,
    xs_sem, xr_sem, rs_send, rs_recv, ag_send, ag_recv, d2_send, d2_recv,
):
    rows_here, columns, channels = state.shape
    devices = lax.axis_size("space")
    chips = devices // CORES
    me = lax.axis_index("space")
    core = lax.rem(me, CORES)
    chip = me // CORES
    other = 1 - core
    partner = chip * CORES + other
    half = chips // 2
    step = 384 if columns % 384 == 0 else columns
    tiles = [(t * step, step) for t in range(columns // step)]

    def peer(distance):
        return lax.rem(chip + distance, chips) * CORES + core

    barrier = pltpu.get_barrier_semaphore()

    def greet(distance, carry):
        pl.semaphore_signal(barrier, inc=1, device_id={"space": peer(distance)}, device_id_type=MESH)
        return carry

    pl.semaphore_signal(barrier, inc=1, device_id={"space": partner}, device_id_type=MESH)
    lax.fori_loop(1, chips, greet, 0)

    small = [
        (zf_hbm, zf), (tf_hbm.at[me], tf), (pm_hbm, pm), (pin_hbm, pin), (min_hbm, minn),
    ]
    late = [
        (lw_hbm, lw), (bias_hbm, bias), (zi_hbm, zi), (ti_hbm.at[me], ti), (pout_hbm, pout),
        (pmt_hbm, pmt), (mout_hbm, mout), (rh_hbm, rh), (rf_hbm, rf),
    ]
    small_copies = [pltpu.make_async_copy(a, b, small_sem.at[i]) for i, (a, b) in enumerate(small)]
    late_copies = [pltpu.make_async_copy(a, b, late_sem.at[i]) for i, (a, b) in enumerate(late)]
    in_copies = [
        pltpu.make_async_copy(x_hbm.at[h], state.at[h], in_sem.at[h]) for h in range(rows_here)
    ]
    sw_copies = [pltpu.make_async_copy(sw_hbm.at[l], sw.at[l], sw_sem.at[l]) for l in range(LAYERS)]
    for copy in small_copies + in_copies + late_copies + sw_copies:
        copy.start()

    for copy in small_copies:
        copy.wait()
    spread_f = dot(dot(pm[...], tf[...]).astype(BF), pin[...]) * minn[...].astype(F32)
    m2[...] = spread_f.astype(BF).reshape(m2.shape)

    for h in range(rows_here):
        in_copies[h].wait()
        zonal[pl.ds(h * 2 * KX, 2 * KX), :] = dot(zf[...], state[h]).astype(BF)

    def send_partials_to_partner(layer):
        xsend[layer] = dot(m2[other], zonal[...]).astype(BF)
        copy = pltpu.make_async_remote_copy(
            src_ref=xsend.at[layer], dst_ref=xrecv.at[layer], send_sem=xs_sem.at[layer],
            recv_sem=xr_sem.at[layer], device_id={"space": partner}, device_id_type=MESH,
        )
        copy.start()
        return copy

    def reduce_sends(layer, partner_copy):
        mine = dot(m2[core], zonal[...])
        partner_copy.wait()
        mine = mine + xrecv[layer].astype(F32)
        pbuf[layer] = mine.reshape(pbuf.shape[1:]).astype(BF)

        def send(distance):
            pltpu.make_async_remote_copy(
                src_ref=pbuf.at[layer, lax.rem(chip + distance, chips)],
                dst_ref=rbuf.at[layer, distance], send_sem=rs_send.at[layer],
                recv_sem=rs_recv.at[layer], device_id={"space": peer(distance)},
                device_id_type=MESH,
            ).start()

        send(half)

        def body(i, carry):
            send(half - 1 - i)
            send(half + 1 + i)
            return carry

        lax.fori_loop(0, half - 1, body, 0)

    def wait_bytes(ref, sem):
        pltpu.make_async_copy(ref, ref, sem).wait()

    def pointwise(layer):
        row_bias = bias[pl.ds(layer, 1), :].astype(F32)

        def body(h, carry):
            for start, size in tiles:
                value = dot(state[h, pl.ds(start, size), :], lw[layer]) + row_bias
                pw[h, pl.ds(start, size), :] = value
            return carry

        lax.fori_loop(0, rows_here, body, 0)

    def reduce_finish_and_mix(layer):
        wait_bytes(rbuf.at[layer, pl.ds(1, chips - 1)], rs_recv.at[layer])
        total = pbuf[layer, chip].astype(F32)
        total = total + jnp.sum(rbuf[layer, pl.ds(1, chips - 1)].astype(F32), axis=0)
        spectrum = total.astype(BF).astype(F32)
        count = spectrum.shape[0]
        row = lax.broadcasted_iota(jnp.int32, spectrum.shape, 0)
        turned = jnp.where(
            row % 2 == 0, -pltpu.roll(spectrum, count - 1, 0), pltpu.roll(spectrum, 1, 0)
        )
        pieces = []
        for mode in range(count // 2):
            here = row // 2 == mode
            pieces.append(jnp.where(here, spectrum, 0.0))
            pieces.append(jnp.where(here, turned, 0.0))
        left = jnp.concatenate(pieces, axis=1).astype(BF)
        mixed = dot(left, sw[layer].reshape(-1, channels))
        mall[layer, core, chip] = mixed.astype(BF)

    def gather(layer):
        own = mall.at[layer, core, chip]

        def send(distance):
            pltpu.make_async_remote_copy(
                src_ref=own, dst_ref=own, send_sem=ag_send.at[layer],
                recv_sem=ag_recv.at[layer, distance], device_id={"space": peer(distance)},
                device_id_type=MESH,
            ).start()

        def relay(source):
            piece = mall.at[layer, core, source]
            pltpu.make_async_remote_copy(
                src_ref=piece, dst_ref=piece, send_sem=d2_send.at[layer],
                recv_sem=d2_recv.at[layer], device_id={"space": partner}, device_id_type=MESH,
            ).start()

        def pass_on(distance):
            source = lax.rem(chip + chips - distance, chips)
            wait_bytes(mall.at[layer, core, source], ag_recv.at[layer, distance])
            relay(source)

        send(half)

        def send_body(i, carry):
            send(half - 1 - i)
            send(half + 1 + i)
            return carry

        lax.fori_loop(0, half - 1, send_body, 0)
        relay(chip)

        def relay_body(i, carry):
            pass_on(1 + i)
            pass_on(chips - 1 - i)
            return carry

        lax.fori_loop(0, half - 1, relay_body, 0)
        pass_on(half)
        wait_bytes(mall.at[layer, other], d2_recv.at[layer])
        modes = mall[layer].astype(F32).reshape(2 * MODES, channels).astype(BF)
        returned[...] = dot(n2[...], modes).astype(BF)

    for copy in late_copies:
        copy.wait()
    spread_i = dot(dot(pout[...], ti[...]).astype(BF), pmt[...]) * mout[...].astype(F32)
    n2[...] = spread_i.astype(BF)
    pointwise(0)
    for copy in sw_copies:
        copy.wait()
    pl.semaphore_wait(barrier, chips)

    reduce_sends(0, send_partials_to_partner(0))
    reduce_finish_and_mix(0)
    gather(0)

    def finish_body(h, carry):
        back = returned[pl.ds(pl.multiple_of(h * 2 * KX, 2 * KX), 2 * KX), :]
        part = jnp.zeros((2 * KX, channels), F32)
        for start, size in tiles:
            value = dot(zi[pl.ds(start, size), :], back) + pw[h, pl.ds(start, size), :]
            value = gelu(value).astype(BF)
            state[h, pl.ds(start, size), :] = value
            part = part + dot(zf[:, pl.ds(start, size)], value)
        zonal[pl.ds(pl.multiple_of(h * 2 * KX, 2 * KX), 2 * KX), :] = part.astype(BF)
        return carry

    lax.fori_loop(0, rows_here, finish_body, 0)

    reduce_sends(1, send_partials_to_partner(1))
    pointwise(1)
    reduce_finish_and_mix(1)
    gather(1)

    def readout_body(h, carry):
        back = returned[pl.ds(pl.multiple_of(h * 2 * KX, 2 * KX), 2 * KX), :]
        for start, size in tiles:
            value = dot(zi[pl.ds(start, size), :], back) + pw[h, pl.ds(start, size), :]
            value = gelu(value).astype(BF)
            hidden = gelu(dot(value, rh[...])).astype(BF)
            final = lax.dot_general(
                rf[...], hidden, (((1,), (1,)), ((), ())), preferred_element_type=F32
            )
            out_ref[h, :, pl.ds(start, size)] = final.astype(BF)
        return carry

    lax.fori_loop(0, rows_here, readout_body, 0)

    for layer in range(LAYERS):
        wait_bytes(pbuf.at[layer, pl.ds(1, chips - 1)], rs_send.at[layer])
        wait_bytes(rbuf.at[layer, pl.ds(1, chips - 1)], ag_send.at[layer])
        wait_bytes(mall.at[layer, core], d2_send.at[layer])


def per_device(inputs, spectral_weight, local_weight, layer_bias, readout_hidden, readout_final):
    rows_here, columns, channels = inputs.shape
    devices = lax.axis_size("space")
    chips = devices // CORES
    each = MODES // devices
    variables, units = readout_final.shape
    zonal_forward, zonal_inverse = zonal_tables(columns)
    table_f, table_i = meridional_tables(devices, rows_here)
    selections = selection_tables(devices, rows_here)
    bands = rows_here * 2 * KX
    operands = (
        inputs, spectral_weight, local_weight, layer_bias, readout_hidden, readout_final,
        zonal_forward, zonal_inverse, table_f, table_i, *selections,
    )
    vmem = pltpu.VMEM
    like = lambda a, cut=0: vmem(a.shape[cut:], BF)
    result = pl.pallas_call(
        kernel,
        name="operator",
        out_shape=jax.ShapeDtypeStruct((rows_here, variables, columns), BF),
        in_specs=[pl.BlockSpec(memory_space=pltpu.HBM)] * len(operands),
        out_specs=pl.BlockSpec(memory_space=pltpu.VMEM),
        scratch_shapes=[
            *[like(a) for a in operands[:8]],
            like(table_f, 1),
            like(table_i, 1),
            *[like(a) for a in selections],
            vmem((CORES, MODES, bands), BF),
            vmem((bands, 2 * MODES), BF),
            vmem((bands, channels), BF),
            vmem((rows_here, columns, channels), F32),
            vmem((bands, channels), BF),
            vmem((LAYERS, MODES, channels), BF),
            vmem((LAYERS, MODES, channels), BF),
            vmem((LAYERS, chips, 2 * each, channels), BF),
            vmem((LAYERS, chips, 2 * each, channels), BF),
            vmem((LAYERS, CORES, chips, 2 * each, channels), BF),
            pltpu.SemaphoreType.DMA((rows_here,)),
            pltpu.SemaphoreType.DMA((LAYERS,)),
            pltpu.SemaphoreType.DMA((5,)),
            pltpu.SemaphoreType.DMA((9,)),
            pltpu.SemaphoreType.DMA((LAYERS,)),
            pltpu.SemaphoreType.DMA((LAYERS,)),
            pltpu.SemaphoreType.DMA((LAYERS,)),
            pltpu.SemaphoreType.DMA((LAYERS,)),
            pltpu.SemaphoreType.DMA((LAYERS,)),
            pltpu.SemaphoreType.DMA((LAYERS, chips)),
            pltpu.SemaphoreType.DMA((LAYERS,)),
            pltpu.SemaphoreType.DMA((LAYERS,)),
        ],
        compiler_params=pltpu.CompilerParams(
            collective_id=0, has_side_effects=True, vmem_limit_bytes=60 * 1024 * 1024
        ),
    )(*operands)
    return jnp.transpose(result, (1, 0, 2))


def solution(mesh):
    in_specs = (
        P(("groups", "space"), None, None),
        P(None, "space", None, None, None),
        P(),
        P(),
        P(),
        P(),
    )
    out_specs = P(None, ("groups", "space"), None)
    return jax.shard_map(
        per_device, mesh=mesh, in_specs=in_specs, out_specs=out_specs, check_vma=False
    )
```

```python
import functools

import jax
import jax.numpy as jnp
import numpy as np
from jax import lax
from jax.experimental import pallas as pl
from jax.experimental.pallas import tpu as pltpu
from jax.sharding import PartitionSpec as P

KY = 16
KX = 16
LAYERS = 2
MODES = KY * KX
CORES = 2
BF = jnp.bfloat16
F32 = jnp.float32
MESH = pl.DeviceIdType.MESH


def zonal_tables(columns):
    phase = np.arange(columns)[:, None] * np.arange(1, KX + 1)[None, :] % columns
    angles = np.float32(2.0 * np.pi / columns) * phase.astype(np.float32)
    cosines, sines = np.cos(angles), np.sin(angles)
    forward = np.concatenate([cosines, -sines], axis=1) / np.sqrt(np.float32(columns))
    inverse = np.stack([cosines, -sines], axis=2).reshape(columns, 2 * KX)
    inverse = inverse * np.sqrt(np.float32(2.0 / KX))
    return forward.T.astype(BF), inverse.astype(BF)


def meridional_tables(devices, rows_here):
    height = devices * rows_here
    index = np.arange(KY)
    waves = np.where(index < KY // 2, index, index - KY)
    rows = np.arange(rows_here)[None, :] * devices + np.arange(devices)[:, None]
    phase = waves[None, :, None] * rows[:, None, :] % height
    angles = np.float32(2.0 * np.pi / height) * phase.astype(np.float32)
    cosines, sines = np.cos(angles), np.sin(angles)
    forward = np.stack([np.stack([cosines, sines], -1), np.stack([-sines, cosines], -1)], 2)
    forward = forward / np.sqrt(np.float32(height))
    cos_t, sin_t = cosines.transpose(0, 2, 1), sines.transpose(0, 2, 1)
    inverse = np.stack([np.stack([cos_t, -sin_t], -1), np.stack([sin_t, cos_t], -1)], 2)
    inverse = inverse / np.sqrt(np.float32(KY))
    pairs = 2 * rows_here
    padded_f = np.zeros((devices, 2 * KY, 128), np.float32)
    padded_f[:, :, :pairs] = forward.reshape(devices, 2 * KY, pairs)
    padded_i = np.zeros((devices, -(-pairs // 16) * 16, 128), np.float32)
    padded_i[:, :pairs, : 2 * KY] = inverse.reshape(devices, pairs, 2 * KY)
    return padded_f.astype(BF), padded_i.astype(BF)


def selection_tables(devices, rows_here):
    each = MODES // devices
    chips = devices // CORES
    core, chip, one, part = np.meshgrid(
        np.arange(CORES), np.arange(chips), np.arange(each), np.arange(2), indexing="ij"
    )
    mode = ((chip * CORES + core) * each + one).reshape(-1)
    part = part.reshape(-1)
    wave_y, wave_x = mode // KX, mode % KX
    pick_mode = (wave_y * 2 + part)[:, None] == np.arange(128)[None, :]
    h, r, k = np.meshgrid(np.arange(rows_here), np.arange(2), np.arange(KX), indexing="ij")
    pick_in = np.arange(128)[:, None] == (h * 2 + r).reshape(-1)[None, :]
    mask_in = wave_x[:, None] == k.reshape(-1)[None, :]
    h, k, p = np.meshgrid(np.arange(rows_here), np.arange(KX), np.arange(2), indexing="ij")
    pairs = -(-2 * rows_here // 16) * 16
    pick_out = (h * 2 + p).reshape(-1)[:, None] == np.arange(pairs)[None, :]
    mask_out = k.reshape(-1)[:, None] == wave_x[None, :]
    tables = (pick_mode[:, : 2 * KY], pick_in, mask_in, pick_out, pick_mode.T, mask_out)
    return tuple(np.asarray(t, np.float32).astype(BF) for t in tables)


def dot(a, b):
    return jnp.dot(a, b, preferred_element_type=F32)


def gelu(v):
    half = 0.5 * v
    scale = float(np.sqrt(2.0 / np.pi))
    return half + half * jnp.tanh(v * (scale + (scale * 0.044715) * (v * v)))


def routes(chips):
    half = chips // 2
    hubs = [h for h in (10, 5) if h + 2 < half]
    reach = (2, -2, 1, -1)
    covered = {h + w for h in hubs for w in (-2, -1, 0, 1, 2)}
    direct = [half] + [s * d for d in range(half - 1, 0, -1) if d not in covered for s in (1, -1)]
    return direct, [s * h for h in hubs for s in (1, -1)], reach


def kernel(
    x_hbm, sw_hbm, lw_hbm, bias_hbm, rh_hbm, rf_hbm, zf_hbm, zi_hbm, tf_hbm, ti_hbm,
    pm_hbm, pin_hbm, min_hbm, pout_hbm, pmt_hbm, mout_hbm,
    out_ref,
    state, sw, lw, bias, rh, rf, zf, zi, tf, ti, pm, pin, minn, pout, pmt, mout,
    m2, n2, zonal, pw, returned, xsend, xrecv, pbuf, rbuf, cbuf, hbuf, mall,
    in_sem, sw_sem, small_sem, late_sem,
    xs_sem, xr_sem, rs_send, rs_stage, rs_recv, ag_send, ag_recv, d2_send, d2_recv,
):
    rows_here, columns, channels = state.shape
    devices = lax.axis_size("space")
    chips = devices // CORES
    me = lax.axis_index("space")
    core = lax.rem(me, CORES)
    chip = me // CORES
    other = 1 - core
    partner = chip * CORES + other
    direct, hubs, reach = routes(chips)
    far = [d for d in direct if abs(d) > max(map(abs, hubs), default=0)]
    near = [d for d in direct if d not in far]
    final_slot = {d: i for i, d in enumerate(direct + hubs)}
    step = 384 if columns % 384 == 0 else columns
    tiles = [(t * step, step) for t in range(columns // step)]

    def chip_at(distance):
        return lax.rem(chip + distance + chips, chips)

    def peer(distance):
        return chip_at(distance) * CORES + core

    barrier = pltpu.get_barrier_semaphore()

    greeted = [peer(d) for d in direct + hubs] + [partner]
    for target in greeted:
        pl.semaphore_signal(barrier, inc=1, device_id={"space": target}, device_id_type=MESH)

    small = [
        (zf_hbm, zf), (tf_hbm.at[me], tf), (pm_hbm, pm), (pin_hbm, pin), (min_hbm, minn),
    ]
    late = [
        (lw_hbm, lw), (bias_hbm, bias), (zi_hbm, zi), (ti_hbm.at[me], ti), (pout_hbm, pout),
        (pmt_hbm, pmt), (mout_hbm, mout), (rh_hbm, rh), (rf_hbm, rf),
    ]
    small_copies = [pltpu.make_async_copy(a, b, small_sem.at[i]) for i, (a, b) in enumerate(small)]
    late_copies = [pltpu.make_async_copy(a, b, late_sem.at[i]) for i, (a, b) in enumerate(late)]
    in_copies = [
        pltpu.make_async_copy(x_hbm.at[h], state.at[h], in_sem.at[h]) for h in range(rows_here)
    ]
    sw_copies = [pltpu.make_async_copy(sw_hbm.at[l], sw.at[l], sw_sem.at[l]) for l in range(LAYERS)]
    for copy in small_copies + in_copies + late_copies + sw_copies:
        copy.start()

    for copy in small_copies:
        copy.wait()
    spread_f = dot(dot(pm[...], tf[...]).astype(BF), pin[...]) * minn[...].astype(F32)
    m2[...] = spread_f.astype(BF).reshape(m2.shape)

    for h in range(rows_here):
        in_copies[h].wait()
        zonal[pl.ds(h * 2 * KX, 2 * KX), :] = dot(zf[...], state[h]).astype(BF)

    def send_partials_to_partner(layer):
        xsend[layer] = dot(m2[other], zonal[...]).astype(BF)
        copy = pltpu.make_async_remote_copy(
            src_ref=xsend.at[layer], dst_ref=xrecv.at[layer], send_sem=xs_sem.at[layer],
            recv_sem=xr_sem.at[layer], device_id={"space": partner}, device_id_type=MESH,
        )
        copy.start()
        return copy

    def reduce_sends(layer, partner_copy):
        mine = dot(m2[core], zonal[...])
        partner_copy.wait()
        mine = mine + xrecv[layer].astype(F32)
        pbuf[layer] = mine.reshape(pbuf.shape[1:]).astype(BF)

        def send(distance):
            pltpu.make_async_remote_copy(
                src_ref=pbuf.at[layer, chip_at(distance)],
                dst_ref=rbuf.at[layer, final_slot[distance]], send_sem=rs_send.at[layer],
                recv_sem=rs_recv.at[layer], device_id={"space": peer(distance)},
                device_id_type=MESH,
            ).start()

        def stage(hub):
            index = hubs.index(hub)
            for slot, offset in enumerate(reach):
                pltpu.make_async_remote_copy(
                    src_ref=pbuf.at[layer, chip_at(offset + hub)],
                    dst_ref=cbuf.at[layer, index, slot], send_sem=rs_send.at[layer],
                    recv_sem=rs_stage.at[layer, index], device_id={"space": peer(offset)},
                    device_id_type=MESH,
                ).start()

        for distance in far[:3]:
            send(distance)
        for hub in hubs[:2]:
            stage(hub)
        for distance in far[3:]:
            send(distance)
        for hub in hubs[2:]:
            stage(hub)
        for distance in near:
            send(distance)

    def reduce_hubs(layer):
        for index, hub in enumerate(hubs):
            wait_bytes(cbuf.at[layer, index], rs_stage.at[layer, index])
            total = pbuf[layer, chip_at(hub)].astype(F32)
            total = total + jnp.sum(cbuf[layer, index].astype(F32), axis=0)
            hbuf[layer, index] = total.astype(BF)
            pltpu.make_async_remote_copy(
                src_ref=hbuf.at[layer, index], dst_ref=rbuf.at[layer, final_slot[hub]],
                send_sem=rs_send.at[layer], recv_sem=rs_recv.at[layer],
                device_id={"space": peer(hub)}, device_id_type=MESH,
            ).start()

    def wait_bytes(ref, sem):
        pltpu.make_async_copy(ref, ref, sem).wait()

    def pointwise(layer):
        row_bias = bias[pl.ds(layer, 1), :].astype(F32)

        def body(h, carry):
            for start, size in tiles:
                value = dot(state[h, pl.ds(start, size), :], lw[layer]) + row_bias
                pw[h, pl.ds(start, size), :] = value
            return carry

        lax.fori_loop(0, rows_here, body, 0)

    def reduce_finish_and_mix(layer):
        wait_bytes(rbuf.at[layer], rs_recv.at[layer])
        total = pbuf[layer, chip].astype(F32)
        total = total + jnp.sum(rbuf[layer].astype(F32), axis=0)
        spectrum = total.astype(BF).astype(F32)
        count = spectrum.shape[0]
        row = lax.broadcasted_iota(jnp.int32, spectrum.shape, 0)
        turned = jnp.where(
            row % 2 == 0, -pltpu.roll(spectrum, count - 1, 0), pltpu.roll(spectrum, 1, 0)
        )
        pieces = []
        for mode in range(count // 2):
            here = row // 2 == mode
            pieces.append(jnp.where(here, spectrum, 0.0))
            pieces.append(jnp.where(here, turned, 0.0))
        left = jnp.concatenate(pieces, axis=1).astype(BF)
        mixed = dot(left, sw[layer].reshape(-1, channels))
        mall[layer, core, chip] = mixed.astype(BF)

    def gather(layer):
        own = mall.at[layer, core, chip]

        def send(piece, target, distance):
            pltpu.make_async_remote_copy(
                src_ref=piece, dst_ref=piece, send_sem=ag_send.at[layer],
                recv_sem=ag_recv.at[layer, distance % chips],
                device_id={"space": peer(target)}, device_id_type=MESH,
            ).start()

        def relay(piece):
            pltpu.make_async_remote_copy(
                src_ref=piece, dst_ref=piece, send_sem=d2_send.at[layer],
                recv_sem=d2_recv.at[layer], device_id={"space": partner}, device_id_type=MESH,
            ).start()

        def arrived(distance):
            piece = mall.at[layer, core, chip_at(-distance)]
            wait_bytes(piece, ag_recv.at[layer, distance % chips])
            return piece

        for distance in far[:3] + hubs[:2] + far[3:] + hubs[2:] + near:
            send(own, distance, distance)
        relay(own)
        for distance in reversed(near):
            relay(arrived(distance))
        for hub in hubs[2:] + hubs[:2]:
            piece = arrived(hub)
            for offset in reach:
                send(piece, offset, hub + offset)
            relay(piece)
        behind = far[:0:-1]
        for hub in hubs[2:]:
            for offset in reach:
                relay(arrived(hub + offset))
        for distance in behind[:4]:
            relay(arrived(distance))
        for hub in hubs[:2]:
            for offset in reach:
                relay(arrived(hub + offset))
        for distance in behind[4:] + far[:1]:
            relay(arrived(distance))
        wait_bytes(mall.at[layer, other], d2_recv.at[layer])
        modes = mall[layer].astype(F32).reshape(2 * MODES, channels).astype(BF)
        returned[...] = dot(n2[...], modes).astype(BF)

    for copy in late_copies:
        copy.wait()
    spread_i = dot(dot(pout[...], ti[...]).astype(BF), pmt[...]) * mout[...].astype(F32)
    n2[...] = spread_i.astype(BF)
    for copy in sw_copies:
        copy.wait()
    pl.semaphore_wait(barrier, len(greeted))

    reduce_sends(0, send_partials_to_partner(0))
    pointwise(0)
    reduce_hubs(0)
    reduce_finish_and_mix(0)
    gather(0)

    def finish_body(h, carry):
        back = returned[pl.ds(pl.multiple_of(h * 2 * KX, 2 * KX), 2 * KX), :]
        part = jnp.zeros((2 * KX, channels), F32)
        for start, size in tiles:
            value = dot(zi[pl.ds(start, size), :], back) + pw[h, pl.ds(start, size), :]
            value = gelu(value).astype(BF)
            state[h, pl.ds(start, size), :] = value
            part = part + dot(zf[:, pl.ds(start, size)], value)
        zonal[pl.ds(pl.multiple_of(h * 2 * KX, 2 * KX), 2 * KX), :] = part.astype(BF)
        return carry

    lax.fori_loop(0, rows_here, finish_body, 0)

    reduce_sends(1, send_partials_to_partner(1))
    pointwise(1)
    reduce_hubs(1)
    reduce_finish_and_mix(1)
    gather(1)

    def readout_body(h, carry):
        back = returned[pl.ds(pl.multiple_of(h * 2 * KX, 2 * KX), 2 * KX), :]
        for start, size in tiles:
            value = dot(zi[pl.ds(start, size), :], back) + pw[h, pl.ds(start, size), :]
            value = gelu(value).astype(BF)
            hidden = gelu(dot(value, rh[...])).astype(BF)
            final = lax.dot_general(
                rf[...], hidden, (((1,), (1,)), ((), ())), preferred_element_type=F32
            )
            out_ref[h, :, pl.ds(start, size)] = final.astype(BF)
        return carry

    lax.fori_loop(0, rows_here, readout_body, 0)

    for layer in range(LAYERS):
        wait_bytes(pbuf.at[layer, pl.ds(1, chips - 1)], rs_send.at[layer])
        wait_bytes(pbuf.at[layer, pl.ds(1, chips - 1)], ag_send.at[layer])
        wait_bytes(mall.at[layer, core], d2_send.at[layer])


def per_device(inputs, spectral_weight, local_weight, layer_bias, readout_hidden, readout_final):
    rows_here, columns, channels = inputs.shape
    devices = lax.axis_size("space")
    chips = devices // CORES
    each = MODES // devices
    direct, hubs, reach = routes(chips)
    variables, units = readout_final.shape
    zonal_forward, zonal_inverse = zonal_tables(columns)
    table_f, table_i = meridional_tables(devices, rows_here)
    selections = selection_tables(devices, rows_here)
    bands = rows_here * 2 * KX
    operands = (
        inputs, spectral_weight, local_weight, layer_bias, readout_hidden, readout_final,
        zonal_forward, zonal_inverse, table_f, table_i, *selections,
    )
    vmem = pltpu.VMEM
    like = lambda a, cut=0: vmem(a.shape[cut:], BF)
    result = pl.pallas_call(
        kernel,
        name="operator",
        out_shape=jax.ShapeDtypeStruct((rows_here, variables, columns), BF),
        in_specs=[pl.BlockSpec(memory_space=pltpu.HBM)] * len(operands),
        out_specs=pl.BlockSpec(memory_space=pltpu.VMEM),
        scratch_shapes=[
            *[like(a) for a in operands[:8]],
            like(table_f, 1),
            like(table_i, 1),
            *[like(a) for a in selections],
            vmem((CORES, MODES, bands), BF),
            vmem((bands, 2 * MODES), BF),
            vmem((bands, channels), BF),
            vmem((rows_here, columns, channels), F32),
            vmem((bands, channels), BF),
            vmem((LAYERS, MODES, channels), BF),
            vmem((LAYERS, MODES, channels), BF),
            vmem((LAYERS, chips, 2 * each, channels), BF),
            vmem((LAYERS, len(direct) + len(hubs), 2 * each, channels), BF),
            vmem((LAYERS, len(hubs), len(reach), 2 * each, channels), BF),
            vmem((LAYERS, len(hubs), 2 * each, channels), BF),
            vmem((LAYERS, CORES, chips, 2 * each, channels), BF),
            pltpu.SemaphoreType.DMA((rows_here,)),
            pltpu.SemaphoreType.DMA((LAYERS,)),
            pltpu.SemaphoreType.DMA((5,)),
            pltpu.SemaphoreType.DMA((9,)),
            pltpu.SemaphoreType.DMA((LAYERS,)),
            pltpu.SemaphoreType.DMA((LAYERS,)),
            pltpu.SemaphoreType.DMA((LAYERS,)),
            pltpu.SemaphoreType.DMA((LAYERS, len(hubs))),
            pltpu.SemaphoreType.DMA((LAYERS,)),
            pltpu.SemaphoreType.DMA((LAYERS,)),
            pltpu.SemaphoreType.DMA((LAYERS, chips)),
            pltpu.SemaphoreType.DMA((LAYERS,)),
            pltpu.SemaphoreType.DMA((LAYERS,)),
        ],
        compiler_params=pltpu.CompilerParams(
            collective_id=0, has_side_effects=True, vmem_limit_bytes=50 * 1024 * 1024
        ),
    )(*[pltpu.with_memory_space_constraint(jnp.asarray(a), pltpu.HBM) for a in operands])
    return jnp.transpose(result, (1, 0, 2))


def solution(mesh):
    in_specs = (
        P(("groups", "space"), None, None),
        P(None, "space", None, None, None),
        P(),
        P(),
        P(),
        P(),
    )
    out_specs = P(None, ("groups", "space"), None)
    return jax.shard_map(
        per_device, mesh=mesh, in_specs=in_specs, out_specs=out_specs, check_vma=False
    )
```

```python
import functools

import jax
import jax.numpy as jnp
import numpy as np
from jax import lax
from jax.experimental import pallas as pl
from jax.experimental.pallas import tpu as pltpu
from jax.sharding import PartitionSpec as P

KY = 16
KX = 16
LAYERS = 2
MODES = KY * KX
CORES = 2
BF = jnp.bfloat16
F32 = jnp.float32
MESH = pl.DeviceIdType.MESH


def zonal_tables(columns):
    phase = np.arange(columns)[:, None] * np.arange(1, KX + 1)[None, :] % columns
    angles = np.float32(2.0 * np.pi / columns) * phase.astype(np.float32)
    cosines, sines = np.cos(angles), np.sin(angles)
    forward = np.concatenate([cosines, -sines], axis=1) / np.sqrt(np.float32(columns))
    inverse = np.stack([cosines, -sines], axis=2).reshape(columns, 2 * KX)
    inverse = inverse * np.sqrt(np.float32(2.0 / KX))
    return forward.T.astype(BF), (0.5 * inverse).astype(BF)


def meridional_tables(devices, rows_here):
    height = devices * rows_here
    index = np.arange(KY)
    waves = np.where(index < KY // 2, index, index - KY)
    rows = np.arange(rows_here)[None, :] * devices + np.arange(devices)[:, None]
    phase = waves[None, :, None] * rows[:, None, :] % height
    angles = np.float32(2.0 * np.pi / height) * phase.astype(np.float32)
    cosines, sines = np.cos(angles), np.sin(angles)
    forward = np.stack([np.stack([cosines, sines], -1), np.stack([-sines, cosines], -1)], 2)
    forward = forward / np.sqrt(np.float32(height))
    cos_t, sin_t = cosines.transpose(0, 2, 1), sines.transpose(0, 2, 1)
    inverse = np.stack([np.stack([cos_t, -sin_t], -1), np.stack([sin_t, cos_t], -1)], 2)
    inverse = inverse / np.sqrt(np.float32(KY))
    pairs = 2 * rows_here
    padded_f = np.zeros((devices, 2 * KY, 128), np.float32)
    padded_f[:, :, :pairs] = forward.reshape(devices, 2 * KY, pairs)
    padded_i = np.zeros((devices, -(-pairs // 16) * 16, 128), np.float32)
    padded_i[:, :pairs, : 2 * KY] = inverse.reshape(devices, pairs, 2 * KY)
    return padded_f.astype(BF), padded_i.astype(BF)


def selection_tables(devices, rows_here):
    each = MODES // devices
    chips = devices // CORES
    core, chip, one, part = np.meshgrid(
        np.arange(CORES), np.arange(chips), np.arange(each), np.arange(2), indexing="ij"
    )
    mode = ((chip * CORES + core) * each + one).reshape(-1)
    part = part.reshape(-1)
    wave_y, wave_x = mode // KX, mode % KX
    pick_mode = (wave_y * 2 + part)[:, None] == np.arange(128)[None, :]
    h, r, k = np.meshgrid(np.arange(rows_here), np.arange(2), np.arange(KX), indexing="ij")
    pick_in = np.arange(128)[:, None] == (h * 2 + r).reshape(-1)[None, :]
    mask_in = wave_x[:, None] == k.reshape(-1)[None, :]
    h, k, p = np.meshgrid(np.arange(rows_here), np.arange(KX), np.arange(2), indexing="ij")
    pairs = -(-2 * rows_here // 16) * 16
    pick_out = (h * 2 + p).reshape(-1)[:, None] == np.arange(pairs)[None, :]
    mask_out = k.reshape(-1)[:, None] == wave_x[None, :]
    tables = (pick_mode[:, : 2 * KY], pick_in, mask_in, pick_out, pick_mode.T, mask_out)
    return tuple(np.asarray(t, np.float32).astype(BF) for t in tables)


def dot(a, b):
    return jnp.dot(a, b, preferred_element_type=F32)


def gelu_of_half(h):
    h = h.astype(BF)
    scale = float(np.sqrt(2.0 / np.pi))
    return h + h * jnp.tanh(h * (2.0 * scale + (8.0 * scale * 0.044715) * (h * h)))


def routes(chips):
    half = chips // 2
    reach = (2, -2, 1, -1)
    hubs = [(s * h, reach) for h in (10, 5) for s in (1, -1) if h + 2 < half]
    covered = {h + w for h, _ in hubs for w in (-2, -1, 0, 1, 2)}
    direct = [half] + [s * d for d in range(half - 1, 0, -1) if d not in covered for s in (1, -1)]
    return direct, hubs


def short_routes(chips):
    half = chips // 2
    quarter = half // 2
    start = quarter // 2
    ahead = [d - quarter for d in range(half, start - 1, -1) if d != quarter]
    behind = [quarter - d for d in range(half - 1, start - 1, -1) if d != quarter]
    direct = [s * d for d in range(start - 1, 0, -1) for s in (1, -1)]
    return direct, [(quarter, tuple(ahead)), (-quarter, tuple(behind))]


def sending_order(direct, hubs):
    staged = [(i, j) for j in range(max(len(w) for _, w in hubs)) for i, (_, w) in enumerate(hubs) if j < len(w)]
    outer = max(abs(h) for h, _ in hubs)
    far = [(d,) for d in direct if abs(d) > outer]
    near = [(d,) for d in direct if abs(d) <= outer]
    first = [s for s in staged if abs(hubs[s[0]][0]) == outer]
    rest = [s for s in staged if s not in first]
    return far[:3] + first + far[3:] + rest + near


def kernel(
    x_hbm, sw_hbm, lw_hbm, bias_hbm, rh_hbm, rf_hbm, zf_hbm, zi_hbm, tf_hbm, ti_hbm,
    pm_hbm, pin_hbm, min_hbm, pout_hbm, pmt_hbm, mout_hbm,
    out_ref,
    state, sw, lw, bias, rh, rf, zf, zi, tf, ti, pm, pin, minn, pout, pmt, mout,
    m2, n2, zonal, pw, returned, xsend, xrecv, pbuf, rbuf_0, cbuf_0, hbuf_0, rbuf_1, cbuf_1, hbuf_1, mall,
    in_sem, sw_sem, small_sem, late_sem,
    xs_sem, xr_sem, rs_send, rs_stage, rs_recv, ag_send, ag_recv, d2_send, d2_recv,
):
    rows_here, columns, channels = state.shape
    devices = lax.axis_size("space")
    chips = devices // CORES
    me = lax.axis_index("space")
    core = lax.rem(me, CORES)
    chip = me // CORES
    other = 1 - core
    partner = chip * CORES + other
    plans = (short_routes(chips), routes(chips))
    landing = ((rbuf_0, cbuf_0, hbuf_0), (rbuf_1, cbuf_1, hbuf_1))
    direct, hub_windows = plans[1]
    hubs = [h for h, _ in hub_windows]
    reach = hub_windows[0][1]
    far = [d for d in direct if abs(d) > max(map(abs, hubs))]
    near = [d for d in direct if d not in far]
    step = 384 if columns % 384 == 0 else columns
    tiles = [(t * step, step) for t in range(columns // step)]

    def chip_at(distance):
        return lax.rem(chip + distance + chips, chips)

    def peer(distance):
        return chip_at(distance) * CORES + core

    barrier = pltpu.get_barrier_semaphore()

    closest = max(abs(d) for hub, window in plans[0][1] for d in (hub, *window))
    greeted = [peer(s * d) for d in range(1, closest + 1) for s in (1, -1)] + [partner]
    for target in greeted:
        pl.semaphore_signal(barrier, inc=1, device_id={"space": target}, device_id_type=MESH)

    small = [
        (zf_hbm, zf), (tf_hbm.at[me], tf), (pm_hbm, pm), (pin_hbm, pin), (min_hbm, minn),
    ]
    late = [
        (lw_hbm, lw), (bias_hbm, bias), (zi_hbm, zi), (ti_hbm.at[me], ti), (pout_hbm, pout),
        (pmt_hbm, pmt), (mout_hbm, mout), (rh_hbm, rh), (rf_hbm, rf),
    ]
    small_copies = [pltpu.make_async_copy(a, b, small_sem.at[i]) for i, (a, b) in enumerate(small)]
    late_copies = [pltpu.make_async_copy(a, b, late_sem.at[i]) for i, (a, b) in enumerate(late)]
    in_copies = [
        pltpu.make_async_copy(x_hbm.at[h], state.at[h], in_sem.at[h]) for h in range(rows_here)
    ]
    sw_copies = [pltpu.make_async_copy(sw_hbm.at[l], sw.at[l], sw_sem.at[l]) for l in range(LAYERS)]
    for copy in small_copies + in_copies + late_copies + sw_copies:
        copy.start()

    for copy in small_copies:
        copy.wait()
    spread_f = dot(dot(pm[...], tf[...]).astype(BF), pin[...]) * minn[...].astype(F32)
    m2[...] = spread_f.astype(BF).reshape(m2.shape)

    for h in range(rows_here):
        in_copies[h].wait()
        zonal[pl.ds(h * 2 * KX, 2 * KX), :] = dot(zf[...], state[h]).astype(BF)

    def send_partials_to_partner(layer):
        xsend[layer] = dot(m2[other], zonal[...]).astype(BF)
        copy = pltpu.make_async_remote_copy(
            src_ref=xsend.at[layer], dst_ref=xrecv.at[layer], send_sem=xs_sem.at[layer],
            recv_sem=xr_sem.at[layer], device_id={"space": partner}, device_id_type=MESH,
        )
        copy.start()
        return copy

    def reduce_sends(layer, partner_copy):
        mine = dot(m2[core], zonal[...])
        partner_copy.wait()
        mine = mine + xrecv[layer].astype(F32)
        pbuf[layer] = mine.reshape(pbuf.shape[1:]).astype(BF)

        whole, staged = plans[layer]
        rbuf, cbuf, _ = landing[layer]
        for step in sending_order(whole, staged):
            if len(step) == 1:
                source, target = chip_at(step[0]), step[0]
                place, semaphore = rbuf.at[whole.index(step[0])], rs_recv.at[layer]
            else:
                index, slot = step
                hub, window = staged[index]
                source, target = chip_at(window[slot] + hub), window[slot]
                place, semaphore = cbuf.at[index, slot], rs_stage.at[layer, index]
            pltpu.make_async_remote_copy(
                src_ref=pbuf.at[layer, source], dst_ref=place, send_sem=rs_send.at[layer],
                recv_sem=semaphore, device_id={"space": peer(target)}, device_id_type=MESH,
            ).start()

    def reduce_hubs(layer):
        whole, staged = plans[layer]
        rbuf, cbuf, hbuf = landing[layer]
        for index, (hub, window) in enumerate(staged):
            pieces = cbuf.at[index, pl.ds(0, len(window))]
            wait_bytes(pieces, rs_stage.at[layer, index])
            total = pbuf[layer, chip_at(hub)].astype(F32)
            total = total + jnp.sum(pieces[...].astype(F32), axis=0)
            hbuf[index] = total.astype(BF)
            pltpu.make_async_remote_copy(
                src_ref=hbuf.at[index], dst_ref=rbuf.at[len(whole) + index],
                send_sem=rs_send.at[layer], recv_sem=rs_recv.at[layer],
                device_id={"space": peer(hub)}, device_id_type=MESH,
            ).start()

    def wait_bytes(ref, sem):
        pltpu.make_async_copy(ref, ref, sem).wait()

    def pointwise(layer):
        row_bias = 0.5 * bias[pl.ds(layer, 1), :].astype(F32)
        half_lw = lw[layer] * 0.5

        def body(h, carry):
            for start, size in tiles:
                value = dot(state[h, pl.ds(start, size), :], half_lw) + row_bias
                pw[h, pl.ds(start, size), :] = value
            return carry

        lax.fori_loop(0, rows_here, body, 0)

    def reduce_finish_and_mix(layer):
        rbuf = landing[layer][0]
        wait_bytes(rbuf, rs_recv.at[layer])
        total = pbuf[layer, chip].astype(F32)
        total = total + jnp.sum(rbuf[...].astype(F32), axis=0)
        spectrum = total.astype(BF).astype(F32)
        count = spectrum.shape[0]
        row = lax.broadcasted_iota(jnp.int32, spectrum.shape, 0)
        turned = jnp.where(
            row % 2 == 0, -pltpu.roll(spectrum, count - 1, 0), pltpu.roll(spectrum, 1, 0)
        )
        pieces = []
        for mode in range(count // 2):
            here = row // 2 == mode
            pieces.append(jnp.where(here, spectrum, 0.0))
            pieces.append(jnp.where(here, turned, 0.0))
        left = jnp.concatenate(pieces, axis=1).astype(BF)
        mixed = dot(left, sw[layer].reshape(-1, channels))
        mall[layer, core, chip] = mixed.astype(BF)

    def gather(layer):
        own = mall.at[layer, core, chip]

        def send(piece, target, distance):
            pltpu.make_async_remote_copy(
                src_ref=piece, dst_ref=piece, send_sem=ag_send.at[layer],
                recv_sem=ag_recv.at[layer, distance % chips],
                device_id={"space": peer(target)}, device_id_type=MESH,
            ).start()

        def relay(piece):
            pltpu.make_async_remote_copy(
                src_ref=piece, dst_ref=piece, send_sem=d2_send.at[layer],
                recv_sem=d2_recv.at[layer], device_id={"space": partner}, device_id_type=MESH,
            ).start()

        def arrived(distance):
            piece = mall.at[layer, core, chip_at(-distance)]
            wait_bytes(piece, ag_recv.at[layer, distance % chips])
            return piece

        for distance in far[:3] + hubs[:2] + far[3:] + hubs[2:] + near:
            send(own, distance, distance)
        relay(own)
        for distance in reversed(near):
            relay(arrived(distance))
        for hub in hubs[2:] + hubs[:2]:
            piece = arrived(hub)
            for offset in reach:
                send(piece, offset, hub + offset)
            relay(piece)
        behind = far[:0:-1]
        for hub in hubs[2:]:
            for offset in reach:
                relay(arrived(hub + offset))
        for distance in behind[:4]:
            relay(arrived(distance))
        for hub in hubs[:2]:
            for offset in reach:
                relay(arrived(hub + offset))
        for distance in behind[4:] + far[:1]:
            relay(arrived(distance))
        wait_bytes(mall.at[layer, other], d2_recv.at[layer])
        modes = mall[layer].astype(F32).reshape(2 * MODES, channels).astype(BF)
        returned[...] = dot(n2[...], modes).astype(BF)

    for copy in late_copies:
        copy.wait()
    spread_i = dot(dot(pout[...], ti[...]).astype(BF), pmt[...]) * mout[...].astype(F32)
    n2[...] = spread_i.astype(BF)
    for copy in sw_copies:
        copy.wait()
    pl.semaphore_wait(barrier, len(greeted))

    reduce_sends(0, send_partials_to_partner(0))
    pointwise(0)
    reduce_hubs(0)
    reduce_finish_and_mix(0)
    gather(0)

    def finish_body(h, carry):
        back = returned[pl.ds(pl.multiple_of(h * 2 * KX, 2 * KX), 2 * KX), :]
        part = jnp.zeros((2 * KX, channels), F32)
        for start, size in tiles:
            value = dot(zi[pl.ds(start, size), :], back) + pw[h, pl.ds(start, size), :]
            value = gelu_of_half(value)
            state[h, pl.ds(start, size), :] = value
            part = part + dot(zf[:, pl.ds(start, size)], value)
        zonal[pl.ds(pl.multiple_of(h * 2 * KX, 2 * KX), 2 * KX), :] = part.astype(BF)
        return carry

    lax.fori_loop(0, rows_here, finish_body, 0)

    reduce_sends(1, send_partials_to_partner(1))
    pointwise(1)
    reduce_hubs(1)
    reduce_finish_and_mix(1)
    gather(1)

    half_rh = rh[...] * 0.5

    def readout_body(h, carry):
        back = returned[pl.ds(pl.multiple_of(h * 2 * KX, 2 * KX), 2 * KX), :]
        for start, size in tiles:
            value = dot(zi[pl.ds(start, size), :], back) + pw[h, pl.ds(start, size), :]
            value = gelu_of_half(value)
            hidden = gelu_of_half(dot(value, half_rh))
            final = lax.dot_general(
                rf[...], hidden, (((1,), (1,)), ((), ())), preferred_element_type=F32
            )
            out_ref[h, :, pl.ds(start, size)] = final.astype(BF)
        return carry

    lax.fori_loop(0, rows_here, readout_body, 0)

    for layer in range(LAYERS):
        wait_bytes(pbuf.at[layer, pl.ds(1, chips - 1)], rs_send.at[layer])
        wait_bytes(pbuf.at[layer, pl.ds(1, chips - 1)], ag_send.at[layer])
        wait_bytes(mall.at[layer, core], d2_send.at[layer])


def per_device(inputs, spectral_weight, local_weight, layer_bias, readout_hidden, readout_final):
    rows_here, columns, channels = inputs.shape
    devices = lax.axis_size("space")
    chips = devices // CORES
    each = MODES // devices
    landings = []
    for direct, hubs in (short_routes(chips), routes(chips)):
        widest = max(len(window) for _, window in hubs)
        landings += [(len(direct) + len(hubs),), (len(hubs), widest), (len(hubs),)]
    variables, units = readout_final.shape
    zonal_forward, zonal_inverse = zonal_tables(columns)
    table_f, table_i = meridional_tables(devices, rows_here)
    selections = selection_tables(devices, rows_here)
    bands = rows_here * 2 * KX
    operands = (
        inputs, spectral_weight, local_weight, layer_bias, readout_hidden, readout_final,
        zonal_forward, zonal_inverse, table_f, table_i, *selections,
    )
    vmem = pltpu.VMEM
    like = lambda a, cut=0: vmem(a.shape[cut:], BF)
    result = pl.pallas_call(
        kernel,
        name="operator",
        out_shape=jax.ShapeDtypeStruct((rows_here, variables, columns), BF),
        in_specs=[pl.BlockSpec(memory_space=pltpu.HBM)] * len(operands),
        out_specs=pl.BlockSpec(memory_space=pltpu.VMEM),
        scratch_shapes=[
            *[like(a) for a in operands[:8]],
            like(table_f, 1),
            like(table_i, 1),
            *[like(a) for a in selections],
            vmem((CORES, MODES, bands), BF),
            vmem((bands, 2 * MODES), BF),
            vmem((bands, channels), BF),
            vmem((rows_here, columns, channels), F32),
            vmem((bands, channels), BF),
            vmem((LAYERS, MODES, channels), BF),
            vmem((LAYERS, MODES, channels), BF),
            vmem((LAYERS, chips, 2 * each, channels), BF),
            *[vmem((*lead, 2 * each, channels), BF) for lead in landings],
            vmem((LAYERS, CORES, chips, 2 * each, channels), BF),
            pltpu.SemaphoreType.DMA((rows_here,)),
            pltpu.SemaphoreType.DMA((LAYERS,)),
            pltpu.SemaphoreType.DMA((5,)),
            pltpu.SemaphoreType.DMA((9,)),
            pltpu.SemaphoreType.DMA((LAYERS,)),
            pltpu.SemaphoreType.DMA((LAYERS,)),
            pltpu.SemaphoreType.DMA((LAYERS,)),
            pltpu.SemaphoreType.DMA((LAYERS, max(lead[0] for lead in landings[2::3]))),
            pltpu.SemaphoreType.DMA((LAYERS,)),
            pltpu.SemaphoreType.DMA((LAYERS,)),
            pltpu.SemaphoreType.DMA((LAYERS, chips)),
            pltpu.SemaphoreType.DMA((LAYERS,)),
            pltpu.SemaphoreType.DMA((LAYERS,)),
        ],
        compiler_params=pltpu.CompilerParams(
            collective_id=0, has_side_effects=True, vmem_limit_bytes=50 * 1024 * 1024
        ),
    )(*[pltpu.with_memory_space_constraint(jnp.asarray(a), pltpu.HBM) for a in operands])
    return jnp.transpose(result, (1, 0, 2))


def solution(mesh):
    in_specs = (
        P(("groups", "space"), None, None),
        P(None, "space", None, None, None),
        P(),
        P(),
        P(),
        P(),
    )
    out_specs = P(None, ("groups", "space"), None)
    return jax.shard_map(
        per_device, mesh=mesh, in_specs=in_specs, out_specs=out_specs, check_vma=False
    )
```

```python
import functools

import jax
import jax.numpy as jnp
import numpy as np
from jax import lax
from jax.experimental import pallas as pl
from jax.experimental.pallas import tpu as pltpu
from jax.sharding import PartitionSpec as P

KY = 16
KX = 16
LAYERS = 2
MODES = KY * KX
CORES = 2
BF = jnp.bfloat16
F32 = jnp.float32
MESH = pl.DeviceIdType.MESH


def zonal_tables(columns):
    phase = np.arange(columns)[:, None] * np.arange(1, KX + 1)[None, :] % columns
    angles = np.float32(2.0 * np.pi / columns) * phase.astype(np.float32)
    cosines, sines = np.cos(angles), np.sin(angles)
    forward = np.concatenate([cosines, -sines], axis=1) / np.sqrt(np.float32(columns))
    inverse = np.stack([cosines, -sines], axis=2).reshape(columns, 2 * KX)
    inverse = inverse * np.sqrt(np.float32(2.0 / KX))
    return forward.T.astype(BF), (0.5 * inverse).astype(BF)


def meridional_tables(devices, rows_here):
    height = devices * rows_here
    index = np.arange(KY)
    waves = np.where(index < KY // 2, index, index - KY)
    rows = np.arange(rows_here)[None, :] * devices + np.arange(devices)[:, None]
    phase = waves[None, :, None] * rows[:, None, :] % height
    angles = np.float32(2.0 * np.pi / height) * phase.astype(np.float32)
    cosines, sines = np.cos(angles), np.sin(angles)
    forward = np.stack([np.stack([cosines, sines], -1), np.stack([-sines, cosines], -1)], 2)
    forward = forward / np.sqrt(np.float32(height))
    cos_t, sin_t = cosines.transpose(0, 2, 1), sines.transpose(0, 2, 1)
    inverse = np.stack([np.stack([cos_t, -sin_t], -1), np.stack([sin_t, cos_t], -1)], 2)
    inverse = inverse / np.sqrt(np.float32(KY))
    pairs = 2 * rows_here
    padded_f = np.zeros((devices, 2 * KY, 128), np.float32)
    padded_f[:, :, :pairs] = forward.reshape(devices, 2 * KY, pairs)
    padded_i = np.zeros((devices, -(-pairs // 16) * 16, 128), np.float32)
    padded_i[:, :pairs, : 2 * KY] = inverse.reshape(devices, pairs, 2 * KY)
    return padded_f.astype(BF), padded_i.astype(BF)


def selection_tables(devices, rows_here):
    each = MODES // devices
    chips = devices // CORES
    core, chip, one, part = np.meshgrid(
        np.arange(CORES), np.arange(chips), np.arange(each), np.arange(2), indexing="ij"
    )
    mode = ((chip * CORES + core) * each + one).reshape(-1)
    part = part.reshape(-1)
    wave_y, wave_x = mode // KX, mode % KX
    pick_mode = (wave_y * 2 + part)[:, None] == np.arange(128)[None, :]
    h, r, k = np.meshgrid(np.arange(rows_here), np.arange(2), np.arange(KX), indexing="ij")
    pick_in = np.arange(128)[:, None] == (h * 2 + r).reshape(-1)[None, :]
    mask_in = wave_x[:, None] == k.reshape(-1)[None, :]
    h, k, p = np.meshgrid(np.arange(rows_here), np.arange(KX), np.arange(2), indexing="ij")
    pairs = -(-2 * rows_here // 16) * 16
    pick_out = (h * 2 + p).reshape(-1)[:, None] == np.arange(pairs)[None, :]
    mask_out = k.reshape(-1)[:, None] == wave_x[None, :]
    tables = (pick_mode[:, : 2 * KY], pick_in, mask_in, pick_out, pick_mode.T, mask_out)
    return tuple(np.asarray(t, np.float32).astype(BF) for t in tables)


def dot(a, b):
    return jnp.dot(a, b, preferred_element_type=F32)


def gelu_of_half(h):
    h = h.astype(BF)
    scale = float(np.sqrt(2.0 / np.pi))
    return h + h * jnp.tanh(h * (2.0 * scale + (8.0 * scale * 0.044715) * (h * h)))


def routes(chips):
    half = chips // 2
    reach = (2, -2, 1, -1)
    hubs = [(s * h, reach) for h in (10, 5) for s in (1, -1) if h + 2 < half]
    covered = {h + w for h, _ in hubs for w in (-2, -1, 0, 1, 2)}
    direct = [half] + [s * d for d in range(half - 1, 0, -1) if d not in covered for s in (1, -1)]
    return direct, hubs


def short_routes(chips):
    half = chips // 2
    near = half // 4
    outer = half - near
    offsets = [s * d for d in range(near, 0, -1) for s in (1, -1)]
    ahead = tuple(offsets)
    behind = tuple(w for w in offsets if w > -near)
    middle = (2, -2, 1, -1)
    hubs = [(outer, ahead), (-outer, behind), (near + 1, middle), (-near - 1, middle)]
    return [2, -2, 1, -1], hubs


def sending_order(direct, hubs):
    staged = [(i, j) for j in range(max(len(w) for _, w in hubs)) for i, (_, w) in enumerate(hubs) if j < len(w)]
    outer = max(abs(h) for h, _ in hubs)
    far = [(d,) for d in direct if abs(d) > outer]
    near = [(d,) for d in direct if abs(d) <= outer]
    first = [s for s in staged if abs(hubs[s[0]][0]) == outer]
    rest = [s for s in staged if s not in first]
    return far[:3] + first + far[3:] + rest + near


def kernel(
    x_hbm, sw_hbm, lw_hbm, bias_hbm, rh_hbm, rf_hbm, zf_hbm, zi_hbm, tf_hbm, ti_hbm,
    pm_hbm, pin_hbm, min_hbm, pout_hbm, pmt_hbm, mout_hbm,
    out_ref,
    state, sw, lw, bias, rh, rf, zf, zi, tf, ti, pm, pin, minn, pout, pmt, mout,
    m2, n2, zonal, pw, returned, xsend, xrecv, pbuf, rbuf_0, cbuf_0, hbuf_0, rbuf_1, cbuf_1, hbuf_1, mall,
    in_sem, sw_sem, small_sem, late_sem,
    xs_sem, xr_sem, rs_send, rs_stage, rs_recv, ag_send, ag_recv, d2_send, d2_recv, chain,
):
    rows_here, columns, channels = state.shape
    devices = lax.axis_size("space")
    chips = devices // CORES
    me = lax.axis_index("space")
    core = lax.rem(me, CORES)
    chip = me // CORES
    other = 1 - core
    partner = chip * CORES + other
    plans = (short_routes(chips), routes(chips))
    landing = ((rbuf_0, cbuf_0, hbuf_0), (rbuf_1, cbuf_1, hbuf_1))
    direct, hub_windows = plans[1]
    hubs = [h for h, _ in hub_windows]
    reach = hub_windows[0][1]
    far = [d for d in direct if abs(d) > max(map(abs, hubs))]
    near = [d for d in direct if d not in far]
    step = 384 if columns % 384 == 0 else columns
    tiles = [(t * step, step) for t in range(columns // step)]

    def chip_at(distance):
        return lax.rem(chip + distance + chips, chips)

    def peer(distance):
        return chip_at(distance) * CORES + core

    barrier = pltpu.get_barrier_semaphore()

    closest = max(abs(d) for _, window in plans[0][1] for d in window)
    greeted = [peer(s * d) for d in range(1, closest + 1) for s in (1, -1)] + [partner]
    for target in greeted:
        pl.semaphore_signal(barrier, inc=1, device_id={"space": target}, device_id_type=MESH)

    small = [
        (zf_hbm, zf), (tf_hbm.at[me], tf), (pm_hbm, pm), (pin_hbm, pin), (min_hbm, minn),
    ]
    late = [
        (lw_hbm, lw), (bias_hbm, bias), (zi_hbm, zi), (ti_hbm.at[me], ti), (pout_hbm, pout),
        (pmt_hbm, pmt), (mout_hbm, mout), (rh_hbm, rh), (rf_hbm, rf),
    ]
    small_copies = [pltpu.make_async_copy(a, b, small_sem.at[i]) for i, (a, b) in enumerate(small)]
    late_copies = [pltpu.make_async_copy(a, b, late_sem.at[i]) for i, (a, b) in enumerate(late)]
    in_copies = [
        pltpu.make_async_copy(x_hbm.at[h], state.at[h], in_sem.at[h]) for h in range(rows_here)
    ]
    sw_copies = [pltpu.make_async_copy(sw_hbm.at[l], sw.at[l], sw_sem.at[l]) for l in range(LAYERS)]
    for copy in small_copies + in_copies:
        copy.start()

    for copy in small_copies:
        copy.wait()
    spread_f = dot(dot(pm[...], tf[...]).astype(BF), pin[...]) * minn[...].astype(F32)
    m2[...] = spread_f.astype(BF).reshape(m2.shape)

    def pass_word(index):
        for side in (closest, -closest):
            pl.semaphore_signal(
                chain.at[index], inc=1, device_id={"space": peer(side)}, device_id_type=MESH
            )

    pl.semaphore_wait(barrier, len(greeted))
    pass_word(0)

    for h in range(rows_here):
        in_copies[h].wait()
        zonal[pl.ds(h * 2 * KX, 2 * KX), :] = dot(zf[...], state[h]).astype(BF)
    for copy in late_copies + sw_copies:
        copy.start()

    def send_partials_to_partner(layer):
        xsend[layer] = dot(m2[other], zonal[...]).astype(BF)
        copy = pltpu.make_async_remote_copy(
            src_ref=xsend.at[layer], dst_ref=xrecv.at[layer], send_sem=xs_sem.at[layer],
            recv_sem=xr_sem.at[layer], device_id={"space": partner}, device_id_type=MESH,
        )
        copy.start()
        return copy

    def reduce_sends(layer, partner_copy):
        mine = dot(m2[core], zonal[...])
        partner_copy.wait()
        mine = mine + xrecv[layer].astype(F32)
        pbuf[layer] = mine.reshape(pbuf.shape[1:]).astype(BF)

        whole, staged = plans[layer]
        rbuf, cbuf, _ = landing[layer]
        for step in sending_order(whole, staged):
            if len(step) == 1:
                source, target = chip_at(step[0]), step[0]
                place, semaphore = rbuf.at[whole.index(step[0])], rs_recv.at[layer]
            else:
                index, slot = step
                hub, window = staged[index]
                source, target = chip_at(window[slot] + hub), window[slot]
                place, semaphore = cbuf.at[index, slot], rs_stage.at[layer, index]
            pltpu.make_async_remote_copy(
                src_ref=pbuf.at[layer, source], dst_ref=place, send_sem=rs_send.at[layer],
                recv_sem=semaphore, device_id={"space": peer(target)}, device_id_type=MESH,
            ).start()

    def reduce_hubs(layer):
        whole, staged = plans[layer]
        rbuf, cbuf, hbuf = landing[layer]
        for index, (hub, window) in enumerate(staged):
            pieces = cbuf.at[index, pl.ds(0, len(window))]
            wait_bytes(pieces, rs_stage.at[layer, index])
            total = pbuf[layer, chip_at(hub)].astype(F32)
            total = total + jnp.sum(pieces[...].astype(F32), axis=0)
            hbuf[index] = total.astype(BF)
            pltpu.make_async_remote_copy(
                src_ref=hbuf.at[index], dst_ref=rbuf.at[len(whole) + index],
                send_sem=rs_send.at[layer], recv_sem=rs_recv.at[layer],
                device_id={"space": peer(hub)}, device_id_type=MESH,
            ).start()

    def wait_bytes(ref, sem):
        pltpu.make_async_copy(ref, ref, sem).wait()

    def pointwise(layer):
        row_bias = 0.5 * bias[pl.ds(layer, 1), :].astype(F32)
        half_lw = lw[layer] * 0.5

        def body(h, carry):
            for start, size in tiles:
                value = dot(state[h, pl.ds(start, size), :], half_lw) + row_bias
                pw[h, pl.ds(start, size), :] = value
            return carry

        lax.fori_loop(0, rows_here, body, 0)

    def reduce_finish_and_mix(layer):
        rbuf = landing[layer][0]
        wait_bytes(rbuf, rs_recv.at[layer])
        total = pbuf[layer, chip].astype(F32)
        total = total + jnp.sum(rbuf[...].astype(F32), axis=0)
        spectrum = total.astype(BF).astype(F32)
        count = spectrum.shape[0]
        row = lax.broadcasted_iota(jnp.int32, spectrum.shape, 0)
        turned = jnp.where(
            row % 2 == 0, -pltpu.roll(spectrum, count - 1, 0), pltpu.roll(spectrum, 1, 0)
        )
        pieces = []
        for mode in range(count // 2):
            here = row // 2 == mode
            pieces.append(jnp.where(here, spectrum, 0.0))
            pieces.append(jnp.where(here, turned, 0.0))
        left = jnp.concatenate(pieces, axis=1).astype(BF)
        mixed = dot(left, sw[layer].reshape(-1, channels))
        mall[layer, core, chip] = mixed.astype(BF)

    def gather(layer):
        own = mall.at[layer, core, chip]

        def send(piece, target, distance):
            pltpu.make_async_remote_copy(
                src_ref=piece, dst_ref=piece, send_sem=ag_send.at[layer],
                recv_sem=ag_recv.at[layer, distance % chips],
                device_id={"space": peer(target)}, device_id_type=MESH,
            ).start()

        def relay(piece):
            pltpu.make_async_remote_copy(
                src_ref=piece, dst_ref=piece, send_sem=d2_send.at[layer],
                recv_sem=d2_recv.at[layer], device_id={"space": partner}, device_id_type=MESH,
            ).start()

        def arrived(distance):
            piece = mall.at[layer, core, chip_at(-distance)]
            wait_bytes(piece, ag_recv.at[layer, distance % chips])
            return piece

        for distance in far[:3] + hubs[:2] + far[3:] + hubs[2:] + near:
            send(own, distance, distance)
        relay(own)
        for distance in reversed(near):
            relay(arrived(distance))
        for hub in hubs[2:] + hubs[:2]:
            piece = arrived(hub)
            for offset in reach:
                send(piece, offset, hub + offset)
            relay(piece)
        behind = far[:0:-1]
        for hub in hubs[2:]:
            for offset in reach:
                relay(arrived(hub + offset))
        for distance in behind[:4]:
            relay(arrived(distance))
        for hub in hubs[:2]:
            for offset in reach:
                relay(arrived(hub + offset))
        for distance in behind[4:] + far[:1]:
            relay(arrived(distance))
        wait_bytes(mall.at[layer, other], d2_recv.at[layer])
        modes = mall[layer].astype(F32).reshape(2 * MODES, channels).astype(BF)
        returned[...] = dot(n2[...], modes).astype(BF)

    reduce_sends(0, send_partials_to_partner(0))
    pl.semaphore_wait(chain.at[0], 2)
    pass_word(1)
    for copy in late_copies:
        copy.wait()
    pointwise(0)
    pl.semaphore_wait(chain.at[1], 2)
    reduce_hubs(0)
    spread_i = dot(dot(pout[...], ti[...]).astype(BF), pmt[...]) * mout[...].astype(F32)
    n2[...] = spread_i.astype(BF)
    for copy in sw_copies:
        copy.wait()
    reduce_finish_and_mix(0)
    gather(0)

    def finish_body(h, carry):
        back = returned[pl.ds(pl.multiple_of(h * 2 * KX, 2 * KX), 2 * KX), :]
        part = jnp.zeros((2 * KX, channels), F32)
        for start, size in tiles:
            value = dot(zi[pl.ds(start, size), :], back) + pw[h, pl.ds(start, size), :]
            value = gelu_of_half(value)
            state[h, pl.ds(start, size), :] = value
            part = part + dot(zf[:, pl.ds(start, size)], value)
        zonal[pl.ds(pl.multiple_of(h * 2 * KX, 2 * KX), 2 * KX), :] = part.astype(BF)
        return carry

    lax.fori_loop(0, rows_here, finish_body, 0)

    reduce_sends(1, send_partials_to_partner(1))
    pointwise(1)
    reduce_hubs(1)
    reduce_finish_and_mix(1)
    gather(1)

    half_rh = rh[...] * 0.5
    spare = jnp.zeros((128 - rf.shape[0], channels), F32)
    rf_t = jnp.concatenate([rf[...].astype(F32), spare], axis=0).T.astype(BF)

    def readout_body(h, carry):
        back = returned[pl.ds(pl.multiple_of(h * 2 * KX, 2 * KX), 2 * KX), :]
        for start, size in tiles:
            value = dot(zi[pl.ds(start, size), :], back) + pw[h, pl.ds(start, size), :]
            value = gelu_of_half(value)
            hidden = gelu_of_half(dot(value, half_rh))
            final = dot(hidden, rf_t)
            out_ref[h, :, pl.ds(start, size)] = final.T[: rf.shape[0]].astype(BF)
        return carry

    lax.fori_loop(0, rows_here, readout_body, 0)

    for layer in range(LAYERS):
        wait_bytes(pbuf.at[layer, pl.ds(1, chips - 1)], rs_send.at[layer])
        wait_bytes(pbuf.at[layer, pl.ds(1, chips - 1)], ag_send.at[layer])
        wait_bytes(mall.at[layer, core], d2_send.at[layer])


def per_device(inputs, spectral_weight, local_weight, layer_bias, readout_hidden, readout_final):
    rows_here, columns, channels = inputs.shape
    devices = lax.axis_size("space")
    chips = devices // CORES
    each = MODES // devices
    landings = []
    for direct, hubs in (short_routes(chips), routes(chips)):
        widest = max(len(window) for _, window in hubs)
        landings += [(len(direct) + len(hubs),), (len(hubs), widest), (len(hubs),)]
    variables, units = readout_final.shape
    zonal_forward, zonal_inverse = zonal_tables(columns)
    table_f, table_i = meridional_tables(devices, rows_here)
    selections = selection_tables(devices, rows_here)
    bands = rows_here * 2 * KX
    operands = (
        inputs, spectral_weight, local_weight, layer_bias, readout_hidden, readout_final,
        zonal_forward, zonal_inverse, table_f, table_i, *selections,
    )
    vmem = pltpu.VMEM
    like = lambda a, cut=0: vmem(a.shape[cut:], BF)
    result = pl.pallas_call(
        kernel,
        name="operator",
        out_shape=jax.ShapeDtypeStruct((rows_here, variables, columns), BF),
        in_specs=[pl.BlockSpec(memory_space=pltpu.HBM)] * len(operands),
        out_specs=pl.BlockSpec(memory_space=pltpu.VMEM),
        scratch_shapes=[
            *[like(a) for a in operands[:8]],
            like(table_f, 1),
            like(table_i, 1),
            *[like(a) for a in selections],
            vmem((CORES, MODES, bands), BF),
            vmem((bands, 2 * MODES), BF),
            vmem((bands, channels), BF),
            vmem((rows_here, columns, channels), F32),
            vmem((bands, channels), BF),
            vmem((LAYERS, MODES, channels), BF),
            vmem((LAYERS, MODES, channels), BF),
            vmem((LAYERS, chips, 2 * each, channels), BF),
            *[vmem((*lead, 2 * each, channels), BF) for lead in landings],
            vmem((LAYERS, CORES, chips, 2 * each, channels), BF),
            pltpu.SemaphoreType.DMA((rows_here,)),
            pltpu.SemaphoreType.DMA((LAYERS,)),
            pltpu.SemaphoreType.DMA((5,)),
            pltpu.SemaphoreType.DMA((9,)),
            pltpu.SemaphoreType.DMA((LAYERS,)),
            pltpu.SemaphoreType.DMA((LAYERS,)),
            pltpu.SemaphoreType.DMA((LAYERS,)),
            pltpu.SemaphoreType.DMA((LAYERS, max(lead[0] for lead in landings[2::3]))),
            pltpu.SemaphoreType.DMA((LAYERS,)),
            pltpu.SemaphoreType.DMA((LAYERS,)),
            pltpu.SemaphoreType.DMA((LAYERS, chips)),
            pltpu.SemaphoreType.DMA((LAYERS,)),
            pltpu.SemaphoreType.DMA((LAYERS,)),
            pltpu.SemaphoreType.REGULAR((2,)),
        ],
        compiler_params=pltpu.CompilerParams(
            collective_id=0, has_side_effects=True, vmem_limit_bytes=50 * 1024 * 1024
        ),
    )(*[pltpu.with_memory_space_constraint(jnp.asarray(a), pltpu.HBM) for a in operands])
    return jnp.transpose(result, (1, 0, 2))


def solution(mesh):
    in_specs = (
        P(("groups", "space"), None, None),
        P(None, "space", None, None, None),
        P(),
        P(),
        P(),
        P(),
    )
    out_specs = P(None, ("groups", "space"), None)
    return jax.shard_map(
        per_device, mesh=mesh, in_specs=in_specs, out_specs=out_specs, check_vma=False
    )
```

```python
import functools

import jax
import jax.numpy as jnp
import numpy as np
from jax import lax
from jax.experimental import pallas as pl
from jax.experimental.pallas import tpu as pltpu
from jax.sharding import PartitionSpec as P

KY = 16
KX = 16
LAYERS = 2
MODES = KY * KX
CORES = 2
BF = jnp.bfloat16
F32 = jnp.float32
MESH = pl.DeviceIdType.MESH


def zonal_tables(columns):
    phase = np.arange(columns)[:, None] * np.arange(1, KX + 1)[None, :] % columns
    angles = np.float32(2.0 * np.pi / columns) * phase.astype(np.float32)
    cosines, sines = np.cos(angles), np.sin(angles)
    forward = np.concatenate([cosines, -sines], axis=1) / np.sqrt(np.float32(columns))
    inverse = np.stack([cosines, -sines], axis=2).reshape(columns, 2 * KX)
    inverse = inverse * np.sqrt(np.float32(2.0 / KX))
    return forward.T.astype(BF), (0.5 * inverse).astype(BF)


def meridional_tables(devices, rows_here):
    height = devices * rows_here
    index = np.arange(KY)
    waves = np.where(index < KY // 2, index, index - KY)
    rows = np.arange(rows_here)[None, :] * devices + np.arange(devices)[:, None]
    phase = waves[None, :, None] * rows[:, None, :] % height
    angles = np.float32(2.0 * np.pi / height) * phase.astype(np.float32)
    cosines, sines = np.cos(angles), np.sin(angles)
    forward = np.stack([np.stack([cosines, sines], -1), np.stack([-sines, cosines], -1)], 2)
    forward = forward / np.sqrt(np.float32(height))
    cos_t, sin_t = cosines.transpose(0, 2, 1), sines.transpose(0, 2, 1)
    inverse = np.stack([np.stack([cos_t, -sin_t], -1), np.stack([sin_t, cos_t], -1)], 2)
    inverse = inverse / np.sqrt(np.float32(KY))
    pairs = 2 * rows_here
    padded_f = np.zeros((devices, 2 * KY, 128), np.float32)
    padded_f[:, :, :pairs] = forward.reshape(devices, 2 * KY, pairs)
    padded_i = np.zeros((devices, -(-pairs // 16) * 16, 128), np.float32)
    padded_i[:, :pairs, : 2 * KY] = inverse.reshape(devices, pairs, 2 * KY)
    return padded_f.astype(BF), padded_i.astype(BF)


def selection_tables(devices, rows_here):
    each = MODES // devices
    chips = devices // CORES
    core, chip, one, part = np.meshgrid(
        np.arange(CORES), np.arange(chips), np.arange(each), np.arange(2), indexing="ij"
    )
    mode = ((chip * CORES + core) * each + one).reshape(-1)
    part = part.reshape(-1)
    wave_y, wave_x = mode // KX, mode % KX
    pick_mode = (wave_y * 2 + part)[:, None] == np.arange(128)[None, :]
    h, r, k = np.meshgrid(np.arange(rows_here), np.arange(2), np.arange(KX), indexing="ij")
    pick_in = np.arange(128)[:, None] == (h * 2 + r).reshape(-1)[None, :]
    mask_in = wave_x[:, None] == k.reshape(-1)[None, :]
    h, k, p = np.meshgrid(np.arange(rows_here), np.arange(KX), np.arange(2), indexing="ij")
    pairs = -(-2 * rows_here // 16) * 16
    pick_out = (h * 2 + p).reshape(-1)[:, None] == np.arange(pairs)[None, :]
    mask_out = k.reshape(-1)[:, None] == wave_x[None, :]
    tables = (pick_mode[:, : 2 * KY], pick_in, mask_in, pick_out, pick_mode.T, mask_out)
    return tuple(np.asarray(t, np.float32).astype(BF) for t in tables)


def dot(a, b):
    return jnp.dot(a, b, preferred_element_type=F32)


def gelu_of_half(h):
    h = h.astype(BF)
    scale = float(np.sqrt(2.0 / np.pi))
    return h + h * jnp.tanh(h * (2.0 * scale + (8.0 * scale * 0.044715) * (h * h)))


def routes(chips):
    half = chips // 2
    reach = (2, -2, 1, -1)
    hubs = [(s * h, reach) for h in (10, 5) for s in (1, -1) if h + 2 < half]
    covered = {h + w for h, _ in hubs for w in (-2, -1, 0, 1, 2)}
    direct = [half] + [s * d for d in range(half - 1, 0, -1) if d not in covered for s in (1, -1)]
    return direct, hubs


def short_routes(chips):
    half = chips // 2
    near = half // 4
    outer = half - near
    offsets = [s * d for d in range(near, 0, -1) for s in (1, -1)]
    ahead = tuple(offsets)
    behind = tuple(w for w in offsets if w > -near)
    middle = (2, -2, 1, -1)
    hubs = [(outer, ahead), (-outer, behind), (near + 1, middle), (-near - 1, middle)]
    return [2, -2, 1, -1], hubs


def sending_order(direct, hubs):
    staged = [(i, j) for j in range(max(len(w) for _, w in hubs)) for i, (_, w) in enumerate(hubs) if j < len(w)]
    outer = max(abs(h) for h, _ in hubs)
    far = [(d,) for d in direct if abs(d) > outer]
    near = [(d,) for d in direct if abs(d) <= outer]
    first = [s for s in staged if abs(hubs[s[0]][0]) == outer]
    rest = [s for s in staged if s not in first]
    return far[:3] + first + far[3:] + rest + near


def kernel(
    x_hbm, sw_hbm, lw_hbm, bias_hbm, rh_hbm, rf_hbm, zf_hbm, zi_hbm, tf_hbm, ti_hbm,
    pm_hbm, pin_hbm, min_hbm, pout_hbm, pmt_hbm, mout_hbm,
    out_ref,
    state, sw, lw, bias, rh, rf, zf, zi, tf, ti, pm, pin, minn, pout, pmt, mout,
    m2, n2, zonal, pw, returned, xsend, xrecv, pbuf, rbuf_0, cbuf_0, hbuf_0, rbuf_1, cbuf_1, hbuf_1, mall,
    in_sem, sw_sem, small_sem, late_sem,
    xs_sem, xr_sem, rs_send, rs_stage, rs_recv, ag_send, ag_recv, d2_send, d2_recv, chain,
):
    rows_here, columns, channels = state.shape
    devices = lax.axis_size("space")
    chips = devices // CORES
    me = lax.axis_index("space")
    core = lax.rem(me, CORES)
    chip = me // CORES
    other = 1 - core
    partner = chip * CORES + other
    plans = (short_routes(chips), routes(chips))
    landing = ((rbuf_0, cbuf_0, hbuf_0), (rbuf_1, cbuf_1, hbuf_1))
    direct, hub_windows = plans[1]
    hubs = [h for h, _ in hub_windows]
    reach = hub_windows[0][1]
    far = [d for d in direct if abs(d) > max(map(abs, hubs))]
    near = [d for d in direct if d not in far]
    grouped = 3 if rows_here % 3 == 0 else 1
    read_tiles = [(r, 0, columns) for r in range(grouped)]

    def chip_at(distance):
        return lax.rem(chip + distance + chips, chips)

    def peer(distance):
        return chip_at(distance) * CORES + core

    barrier = pltpu.get_barrier_semaphore()

    closest = max(abs(d) for _, window in plans[0][1] for d in window)
    greeted = [peer(s * d) for d in range(1, closest + 1) for s in (1, -1)] + [partner]
    for target in greeted:
        pl.semaphore_signal(barrier, inc=1, device_id={"space": target}, device_id_type=MESH)

    small = [
        (zf_hbm, zf), (tf_hbm.at[me], tf), (pm_hbm, pm), (pin_hbm, pin), (min_hbm, minn),
    ]
    late = [
        (lw_hbm, lw), (bias_hbm, bias), (zi_hbm, zi), (ti_hbm.at[me], ti), (pout_hbm, pout),
        (pmt_hbm, pmt), (mout_hbm, mout), (rh_hbm, rh), (rf_hbm, rf),
    ]
    small_copies = [pltpu.make_async_copy(a, b, small_sem.at[i]) for i, (a, b) in enumerate(small)]
    late_copies = [pltpu.make_async_copy(a, b, late_sem.at[i]) for i, (a, b) in enumerate(late)]
    in_copies = [
        pltpu.make_async_copy(x_hbm.at[h], state.at[h], in_sem.at[h]) for h in range(rows_here)
    ]
    sw_copies = [pltpu.make_async_copy(sw_hbm.at[l], sw.at[l], sw_sem.at[l]) for l in range(LAYERS)]
    for copy in small_copies + in_copies:
        copy.start()

    for copy in small_copies:
        copy.wait()
    spread_f = dot(dot(pm[...], tf[...]).astype(BF), pin[...]) * minn[...].astype(F32)
    m2[...] = spread_f.astype(BF).reshape(m2.shape)

    def pass_word(index):
        for side in (closest, -closest):
            pl.semaphore_signal(
                chain.at[index], inc=1, device_id={"space": peer(side)}, device_id_type=MESH
            )

    pl.semaphore_wait(barrier, len(greeted))
    pass_word(0)

    for h in range(rows_here):
        in_copies[h].wait()
        zonal[pl.ds(h * 2 * KX, 2 * KX), :] = dot(zf[...], state[h]).astype(BF)
    for copy in late_copies + sw_copies:
        copy.start()

    def send_partials_to_partner(layer):
        xsend[layer] = dot(m2[other], zonal[...]).astype(BF)
        copy = pltpu.make_async_remote_copy(
            src_ref=xsend.at[layer], dst_ref=xrecv.at[layer], send_sem=xs_sem.at[layer],
            recv_sem=xr_sem.at[layer], device_id={"space": partner}, device_id_type=MESH,
        )
        copy.start()
        return copy

    def reduce_sends(layer, partner_copy):
        mine = dot(m2[core], zonal[...])
        partner_copy.wait()
        mine = mine + xrecv[layer].astype(F32)
        pbuf[layer] = mine.reshape(pbuf.shape[1:]).astype(BF)

        whole, staged = plans[layer]
        rbuf, cbuf, _ = landing[layer]
        for step in sending_order(whole, staged):
            if len(step) == 1:
                source, target = chip_at(step[0]), step[0]
                place, semaphore = rbuf.at[whole.index(step[0])], rs_recv.at[layer]
            else:
                index, slot = step
                hub, window = staged[index]
                source, target = chip_at(window[slot] + hub), window[slot]
                place, semaphore = cbuf.at[index, slot], rs_stage.at[layer, index]
            pltpu.make_async_remote_copy(
                src_ref=pbuf.at[layer, source], dst_ref=place, send_sem=rs_send.at[layer],
                recv_sem=semaphore, device_id={"space": peer(target)}, device_id_type=MESH,
            ).start()

    def reduce_hubs(layer):
        whole, staged = plans[layer]
        rbuf, cbuf, hbuf = landing[layer]
        for index, (hub, window) in enumerate(staged):
            pieces = cbuf.at[index, pl.ds(0, len(window))]
            wait_bytes(pieces, rs_stage.at[layer, index])
            total = pbuf[layer, chip_at(hub)].astype(F32)
            total = total + jnp.sum(pieces[...].astype(F32), axis=0)
            hbuf[index] = total.astype(BF)
            pltpu.make_async_remote_copy(
                src_ref=hbuf.at[index], dst_ref=rbuf.at[len(whole) + index],
                send_sem=rs_send.at[layer], recv_sem=rs_recv.at[layer],
                device_id={"space": peer(hub)}, device_id_type=MESH,
            ).start()

    def wait_bytes(ref, sem):
        pltpu.make_async_copy(ref, ref, sem).wait()

    def pointwise(layer):
        row_bias = 0.5 * bias[pl.ds(layer, 1), :].astype(F32)
        half_lw = lw[layer] * 0.5

        def body(h, carry):
            pw[h] = dot(state[h], half_lw) + row_bias
            return carry

        lax.fori_loop(0, rows_here, body, 0)

    def reduce_finish_and_mix(layer):
        rbuf = landing[layer][0]
        wait_bytes(rbuf, rs_recv.at[layer])
        total = pbuf[layer, chip].astype(F32)
        total = total + jnp.sum(rbuf[...].astype(F32), axis=0)
        spectrum = total.astype(BF).astype(F32)
        count = spectrum.shape[0]
        row = lax.broadcasted_iota(jnp.int32, spectrum.shape, 0)
        turned = jnp.where(
            row % 2 == 0, -pltpu.roll(spectrum, count - 1, 0), pltpu.roll(spectrum, 1, 0)
        )
        pieces = []
        for mode in range(count // 2):
            here = row // 2 == mode
            pieces.append(jnp.where(here, spectrum, 0.0))
            pieces.append(jnp.where(here, turned, 0.0))
        left = jnp.concatenate(pieces, axis=1).astype(BF)
        mixed = dot(left, sw[layer].reshape(-1, channels))
        mall[layer, core, chip] = mixed.astype(BF)

    def gather(layer):
        own = mall.at[layer, core, chip]

        def send(piece, target, distance):
            pltpu.make_async_remote_copy(
                src_ref=piece, dst_ref=piece, send_sem=ag_send.at[layer],
                recv_sem=ag_recv.at[layer, distance % chips],
                device_id={"space": peer(target)}, device_id_type=MESH,
            ).start()

        def relay(piece):
            pltpu.make_async_remote_copy(
                src_ref=piece, dst_ref=piece, send_sem=d2_send.at[layer],
                recv_sem=d2_recv.at[layer], device_id={"space": partner}, device_id_type=MESH,
            ).start()

        def arrived(distance):
            piece = mall.at[layer, core, chip_at(-distance)]
            wait_bytes(piece, ag_recv.at[layer, distance % chips])
            return piece

        for distance in far[:3] + hubs[:2] + far[3:] + hubs[2:] + near:
            send(own, distance, distance)
        relay(own)
        for distance in reversed(near):
            relay(arrived(distance))
        for hub in hubs[2:] + hubs[:2]:
            piece = arrived(hub)
            for offset in reach:
                send(piece, offset, hub + offset)
            relay(piece)
        behind = far[:0:-1]
        for hub in hubs[2:]:
            for offset in reach:
                relay(arrived(hub + offset))
        for distance in behind[:4]:
            relay(arrived(distance))
        for hub in hubs[:2]:
            for offset in reach:
                relay(arrived(hub + offset))
        for distance in behind[4:] + far[:1]:
            relay(arrived(distance))
        def back(side):
            modes = mall[layer, side].astype(F32).reshape(MODES, channels).astype(BF)
            return dot(n2[side], modes)

        back_own = back(core)
        wait_bytes(mall.at[layer, other], d2_recv.at[layer])
        returned[...] = (back_own + back(other)).astype(BF)

    reduce_sends(0, send_partials_to_partner(0))
    pl.semaphore_wait(chain.at[0], 2)
    pass_word(1)
    for copy in late_copies:
        copy.wait()
    pointwise(0)
    pl.semaphore_wait(chain.at[1], 2)
    reduce_hubs(0)
    spread_i = dot(dot(pout[...], ti[...]).astype(BF), pmt[...]) * mout[...].astype(F32)
    for side in range(CORES):
        n2[side] = spread_i[:, side * MODES : (side + 1) * MODES].astype(BF)
    for copy in sw_copies:
        copy.wait()
    reduce_finish_and_mix(0)
    gather(0)

    def finish_body(h, carry):
        band = pl.ds(pl.multiple_of(h * 2 * KX, 2 * KX), 2 * KX)
        value = gelu_of_half(dot(zi[...], returned[band, :]) + pw[h])
        state[h] = value
        zonal[band, :] = dot(zf[...], value).astype(BF)
        return carry

    lax.fori_loop(0, rows_here, finish_body, 0)

    reduce_sends(1, send_partials_to_partner(1))
    pointwise(1)
    reduce_hubs(1)
    reduce_finish_and_mix(1)
    gather(1)

    half_rh = rh[...] * 0.5
    spare = jnp.zeros((128 - rf.shape[0], channels), F32)
    rf_t = jnp.concatenate([rf[...].astype(F32), spare], axis=0).T.astype(BF)

    def readout_body(group, carry):
        values, hiddens = {}, {}

        def first(i):
            r, start, size = read_tiles[i]
            h = group * grouped + r
            back = returned[pl.ds(pl.multiple_of(h * 2 * KX, 2 * KX), 2 * KX), :]
            value = dot(zi[pl.ds(start, size), :], back) + pw[h, pl.ds(start, size), :]
            values[i] = gelu_of_half(value)

        def second(i):
            hiddens[i] = gelu_of_half(dot(values[i], half_rh))

        def third(i):
            r, start, size = read_tiles[i]
            final = dot(hiddens[i], rf_t).T[: rf.shape[0]]
            out_ref[group * grouped + r, :, pl.ds(start, size)] = final.astype(BF)

        count = len(read_tiles)
        for i in range(count + 2):
            if i >= 2:
                third(i - 2)
            if 1 <= i <= count:
                second(i - 1)
            if i < count:
                first(i)
        return carry

    lax.fori_loop(0, rows_here // grouped, readout_body, 0)

    for layer in range(LAYERS):
        wait_bytes(pbuf.at[layer, pl.ds(1, chips - 1)], rs_send.at[layer])
        wait_bytes(pbuf.at[layer, pl.ds(1, chips - 1)], ag_send.at[layer])
        wait_bytes(mall.at[layer, core], d2_send.at[layer])


def per_device(inputs, spectral_weight, local_weight, layer_bias, readout_hidden, readout_final):
    rows_here, columns, channels = inputs.shape
    devices = lax.axis_size("space")
    chips = devices // CORES
    each = MODES // devices
    landings = []
    for direct, hubs in (short_routes(chips), routes(chips)):
        widest = max(len(window) for _, window in hubs)
        landings += [(len(direct) + len(hubs),), (len(hubs), widest), (len(hubs),)]
    variables, units = readout_final.shape
    zonal_forward, zonal_inverse = zonal_tables(columns)
    table_f, table_i = meridional_tables(devices, rows_here)
    selections = selection_tables(devices, rows_here)
    bands = rows_here * 2 * KX
    operands = (
        inputs, spectral_weight, local_weight, layer_bias, readout_hidden, readout_final,
        zonal_forward, zonal_inverse, table_f, table_i, *selections,
    )
    vmem = pltpu.VMEM
    like = lambda a, cut=0: vmem(a.shape[cut:], BF)
    result = pl.pallas_call(
        kernel,
        name="operator",
        out_shape=jax.ShapeDtypeStruct((rows_here, variables, columns), BF),
        in_specs=[pl.BlockSpec(memory_space=pltpu.HBM)] * len(operands),
        out_specs=pl.BlockSpec(memory_space=pltpu.VMEM),
        scratch_shapes=[
            *[like(a) for a in operands[:8]],
            like(table_f, 1),
            like(table_i, 1),
            *[like(a) for a in selections],
            vmem((CORES, MODES, bands), BF),
            vmem((CORES, bands, MODES), BF),
            vmem((bands, channels), BF),
            vmem((rows_here, columns, channels), F32),
            vmem((bands, channels), BF),
            vmem((LAYERS, MODES, channels), BF),
            vmem((LAYERS, MODES, channels), BF),
            vmem((LAYERS, chips, 2 * each, channels), BF),
            *[vmem((*lead, 2 * each, channels), BF) for lead in landings],
            vmem((LAYERS, CORES, chips, 2 * each, channels), BF),
            pltpu.SemaphoreType.DMA((rows_here,)),
            pltpu.SemaphoreType.DMA((LAYERS,)),
            pltpu.SemaphoreType.DMA((5,)),
            pltpu.SemaphoreType.DMA((9,)),
            pltpu.SemaphoreType.DMA((LAYERS,)),
            pltpu.SemaphoreType.DMA((LAYERS,)),
            pltpu.SemaphoreType.DMA((LAYERS,)),
            pltpu.SemaphoreType.DMA((LAYERS, max(lead[0] for lead in landings[2::3]))),
            pltpu.SemaphoreType.DMA((LAYERS,)),
            pltpu.SemaphoreType.DMA((LAYERS,)),
            pltpu.SemaphoreType.DMA((LAYERS, chips)),
            pltpu.SemaphoreType.DMA((LAYERS,)),
            pltpu.SemaphoreType.DMA((LAYERS,)),
            pltpu.SemaphoreType.REGULAR((2,)),
        ],
        compiler_params=pltpu.CompilerParams(
            collective_id=0, has_side_effects=True, vmem_limit_bytes=50 * 1024 * 1024
        ),
    )(*[pltpu.with_memory_space_constraint(jnp.asarray(a), pltpu.HBM) for a in operands])
    return jnp.transpose(result, (1, 0, 2))


def solution(mesh):
    in_specs = (
        P(("groups", "space"), None, None),
        P(None, "space", None, None, None),
        P(),
        P(),
        P(),
        P(),
    )
    out_specs = P(None, ("groups", "space"), None)
    return jax.shard_map(
        per_device, mesh=mesh, in_specs=in_specs, out_specs=out_specs, check_vma=False
    )
```
